256 devices in a mesh: seq: 32 (over z, x), tp: 8 (over y, core).
Axes of the slice: x: 4, y: 4, z: 8, core: 2. Of those that a mesh axis runs over, the one named last changes fastest.
Arguments:
- queries: bfloat16 [8192, 8192], P('seq', 'tp'), may hold values from -120 to 120
- keys: bfloat16 [8192, 1024], P('seq', 'tp'), may hold values from -5 to 5
- values: bfloat16 [8192, 1024], P('seq', 'tp'), may hold values from -6 to 6
- w_query: bfloat16 [8192, 8192], P('seq', 'tp'), may hold values from -0.0625 to 0.0625
- key_weight: bfloat16 [8192, 1024], P('seq'), may hold values from -0.0625 to 0.0625
Outputs:
- attended: bfloat16 [8192, 8192], P('seq', 'tp')
- head_logit_maxima: float32 [64], P('tp')
- w_query_clipped: bfloat16 [8192, 8192], P('seq', 'tp')
- clipped_key_weight: bfloat16 [8192, 1024], P('seq')
The draws below stay inside these ranges and needn't reach their ends.
All inputs are finite; a program needn't handle non-finite values.
Results may differ from the reference program's by a relative error of at most 0.004.
Values may be sent and summed in bfloat16 or wider, within the bound.
A program may use at most 64 MiB of HBM per device.

```python
import math
import jax
import jax.numpy as jnp
from jax import lax

MODEL_WIDTH = 8192
QUERY_HEADS = 64
KEY_VALUE_HEADS = 8
HEAD_SIZE = 128
SEQUENCE_LENGTH = 8192


def random_key_table(key):
    gaussian_sample = jnp.clip(jax.random.normal(jax.random.fold_in(key, 71), (SEQUENCE_LENGTH, KEY_VALUE_HEADS, HEAD_SIZE), jnp.float32), -5.0, 5.0)
    return gaussian_sample


def draw_keys(key, part):
    return random_key_table(key).reshape(SEQUENCE_LENGTH, KEY_VALUE_HEADS * HEAD_SIZE).astype(jnp.bfloat16)


def draw_queries(key, part):
    head_scale = jnp.exp(jax.random.uniform(jax.random.fold_in(key, 72), (QUERY_HEADS,), jnp.float32, math.log(0.3), math.log(3.0)))
    gaussian_sample = jnp.clip(jax.random.normal(jax.random.fold_in(key, 73), (SEQUENCE_LENGTH, QUERY_HEADS, HEAD_SIZE), jnp.float32), -5.0, 5.0)
    gaussian_sample = gaussian_sample * head_scale[None, :, None]
    return gaussian_sample.reshape(SEQUENCE_LENGTH, QUERY_HEADS * HEAD_SIZE).astype(jnp.bfloat16)


def levels(rng, dims, shards, least, top_value):
    loudness = 1.0
    for position, parts in shards:
        draws = jax.random.uniform(jax.random.fold_in(jax.random.fold_in(rng, 6), position), (parts,), jnp.float32, least / len(shards), top_value / len(shards))
        loudness = loudness * jnp.repeat(jnp.exp(draws), dims[position] // parts).reshape((-1,) + (1,) * (len(dims) - 1 - position))
    return loudness


def centred(own_key, dims, width, bound, pieces=(), held_as=jnp.bfloat16):
    factor_of = levels(own_key, dims, pieces, -0.22, 0.18) if pieces else 1.0
    values = jax.random.normal(own_key, dims, jnp.float32) * width * factor_of
    return jnp.minimum(jnp.maximum(values, -bound), bound).astype(held_as)


def setup_inputs(seed: int = 0) -> dict:
    arg_keys = jax.random.split(jax.random.key(seed), 6)
    return {
        "queries": draw_queries(jax.random.fold_in(arg_keys[5], 71), 0),
        "keys": draw_keys(jax.random.fold_in(arg_keys[5], 71), 0),
        "values": centred(arg_keys[2], (SEQUENCE_LENGTH, KEY_VALUE_HEADS * HEAD_SIZE), 1.0, 6.0, ((0, 32), (1, 8))),
        "w_query": centred(arg_keys[3], (MODEL_WIDTH, QUERY_HEADS * HEAD_SIZE), MODEL_WIDTH ** -0.5, 0.0625, ((0, 32), (1, 8))),
        "key_weight": centred(arg_keys[4], (MODEL_WIDTH, KEY_VALUE_HEADS * HEAD_SIZE), MODEL_WIDTH ** -0.5, 0.0625, ((0, 32),)),
    }


clip_threshold = 10.0

def reference(queries, keys, values, w_query, key_weight):
    group_size = QUERY_HEADS // KEY_VALUE_HEADS
    block_rows = math.gcd(SEQUENCE_LENGTH, 512)
    inv_sqrt = HEAD_SIZE ** (-0.5)
    query_heads_view = jnp.moveaxis(queries.reshape(SEQUENCE_LENGTH, KEY_VALUE_HEADS, group_size, HEAD_SIZE), 1, 0)
    key_heads_view = jnp.moveaxis(keys.reshape(SEQUENCE_LENGTH, KEY_VALUE_HEADS, HEAD_SIZE), 1, 0)
    value_heads_view = jnp.moveaxis(values.reshape(SEQUENCE_LENGTH, KEY_VALUE_HEADS, HEAD_SIZE), 1, 0)
    key_positions = jnp.arange(SEQUENCE_LENGTH, dtype=jnp.int32)

    def one_head(operands):
        head_queries, head_keys, head_values = operands
        keys_wide = head_keys.astype(jnp.float32)
        values_wide = head_values.astype(jnp.float32)

        def one_block(running, block_index):
            block_queries = lax.dynamic_slice_in_dim(head_queries, block_index * block_rows, block_rows, 0).astype(jnp.float32)
            scores = jnp.einsum('bgd,nd->bgn', block_queries, keys_wide) * inv_sqrt
            query_positions = block_index * block_rows + jnp.arange(block_rows, dtype=jnp.int32)
            visible = (query_positions[:, None] >= key_positions[None, :])[:, None, :]
            masked = jnp.where(visible, scores, jnp.float32(-1e+30))
            row_max = masked.max(-1)
            expo = jnp.where(visible, jnp.exp(masked - row_max[..., None]), jnp.float32(0.0))
            totals = expo.sum(-1)
            probs = lax.optimization_barrier(expo.astype(jnp.bfloat16)).astype(jnp.float32)
            mixed = jnp.einsum('bgn,nd->bgd', probs, values_wide) / totals[..., None]
            return (jnp.maximum(running, masked.max(axis=(0, 2))), mixed.astype(jnp.bfloat16))
        head_max, block_out = lax.scan(one_block, jnp.full((group_size,), -1e+30, jnp.float32), jnp.arange(SEQUENCE_LENGTH // block_rows, dtype=jnp.int32))
        return (head_max, block_out.reshape(SEQUENCE_LENGTH, group_size, HEAD_SIZE))
    head_max, outputs = lax.map(one_head, (query_heads_view, key_heads_view, value_heads_view))
    attended = jnp.moveaxis(outputs, 0, 1).reshape(SEQUENCE_LENGTH, QUERY_HEADS * HEAD_SIZE)
    head_logit_maxima = head_max.reshape(QUERY_HEADS)
    gamma = clip_threshold / jnp.maximum(head_logit_maxima, clip_threshold)
    clip_logits = clip_threshold / jnp.maximum(head_logit_maxima.reshape(KEY_VALUE_HEADS, group_size).max(1), clip_threshold)
    query_factor = gamma / jnp.sqrt(jnp.repeat(clip_logits, group_size))
    w_query_clipped = (w_query.astype(jnp.float32).reshape(MODEL_WIDTH, QUERY_HEADS, HEAD_SIZE) * query_factor[None, :, None]).reshape(MODEL_WIDTH, QUERY_HEADS * HEAD_SIZE).astype(jnp.bfloat16)
    clipped_key_weight = (key_weight.astype(jnp.float32).reshape(MODEL_WIDTH, KEY_VALUE_HEADS, HEAD_SIZE) * jnp.sqrt(clip_logits)[None, :, None]).reshape(MODEL_WIDTH, KEY_VALUE_HEADS * HEAD_SIZE).astype(jnp.bfloat16)
    return (attended, head_logit_maxima, w_query_clipped, clipped_key_weight)
```

```python
import math

import jax
import jax.numpy as jnp
from jax import lax
from jax.experimental import pallas as pl
from jax.experimental.pallas import tpu as pltpu
from jax.sharding import PartitionSpec as P

HEAD = 128
ROWS = 256
NZ, NX = 8, 4
TAU = 10.0
NEG = -1e30
LOG2_SCALE = math.log2(math.e) / math.sqrt(128.0)
MESH = pl.DeviceIdType.MESH


def attention_kernel(q_hbm, k_hbm, v_hbm, o_hbm, hm_ref,
                     qv, kv, tr, qin, qhl, acc, mrow, res,
                     ld_sem, kv_sem, tr_sem, q_sem, o_sem,
                     zs_sem, xs_sem, ds_sem, qs_sem, os_sem):
    s = lax.axis_index("seq")
    t = lax.axis_index("tp")
    z = s // NX
    x = lax.rem(s, NX)
    c = lax.rem(t, 2)
    ch = z // (NZ // 2)
    driver = c == ch
    foreign = c != ch
    r = z + c * (NZ - 1 - 2 * z)
    rh = z + ch * (NZ - 1 - 2 * z)
    sib = t + 1 - 2 * c
    part = (NZ - 1 - z) * NX + (NX - 1 - x)
    xr = z * NX + lax.rem(x + 1, NX)
    xl = z * NX + lax.rem(x + NX - 1, NX)
    zu_z = lax.rem(z + NZ + 1 - 2 * c, NZ)
    zd_z = lax.rem(z + NZ - 1 + 2 * c, NZ)
    zu = zu_z * NX + x
    zd = zd_z * NX + x
    pu = lax.rem(r + 2, NZ)
    pd = lax.rem(NZ + 5 - r, NZ)

    own_k = pltpu.make_async_copy(k_hbm, kv.at[r, x, 0], ld_sem.at[0])
    own_v = pltpu.make_async_copy(v_hbm, kv.at[r, x, 1], ld_sem.at[1])
    tr_k = pltpu.make_async_copy(k_hbm, tr.at[0, 0], ld_sem.at[0])
    tr_v = pltpu.make_async_copy(v_hbm, tr.at[0, 1], ld_sem.at[1])
    q_lo = pltpu.make_async_copy(q_hbm.at[:, pl.ds(0, 512)], qv.at[0], ld_sem.at[2])
    q_hi = pltpu.make_async_copy(q_hbm.at[:, pl.ds(512, 512)], qv.at[1], ld_sem.at[3])

    @pl.when(driver)
    def _():
        own_k.start()
        own_v.start()

    @pl.when(foreign)
    def _():
        tr_k.start()
        tr_v.start()

    q_lo.start()
    q_hi.start()

    barrier = pltpu.get_barrier_semaphore()
    for dev in ((zu, t), (zd, t), (xr, t), (xl, t), (s, sib), (part, t), (part, sib)):
        pl.semaphore_signal(barrier, inc=1, device_id=dev, device_id_type=MESH)
    pl.semaphore_wait(barrier, 7)

    def remote(src, dst, send, recv, dev):
        return pltpu.make_async_remote_copy(
            src_ref=src, dst_ref=dst, send_sem=send, recv_sem=recv,
            device_id=dev, device_id_type=MESH)

    def blk(row, col):
        return kv.at[row, col]

    def zcopy(row, slot, dev):
        return remote(blk(row, x), blk(row, x), zs_sem.at[slot], kv_sem.at[row, x], (dev, t))

    def xcopy(n, j, row, col, dev):
        return remote(blk(row, col), blk(row, col), xs_sem.at[n, j], kv_sem.at[row, col], (dev, t))

    def dcopy(row, col):
        return remote(blk(row, col), blk(row, col), ds_sem.at[row, col], kv_sem.at[row, col], (s, sib))

    def arrived(row, col):
        pltpu.make_async_copy(blk(row, col), blk(row, col), kv_sem.at[row, col]).wait()

    def order(n):
        nu = rh + 2
        nd = 5 - rh
        m = jnp.minimum(nu, nd)
        k2 = (n + 1) // 2 - 1
        early = n <= 2 * m
        k = jnp.where(early, k2, n - 1 - m)
        from_u = jnp.where(early, lax.rem(n, 2), (nu > nd).astype(jnp.int32)) == 1
        row = jnp.where(from_u, rh + NZ - 1 - k, rh + 1 + k)
        row = jnp.where(n == 0, rh, lax.rem(row, NZ))
        return row, from_u

    xm1 = lax.rem(x + NX - 1, NX)
    xp1 = lax.rem(x + 1, NX)
    xp2 = lax.rem(x + 2, NX)

    def fwd_copies(n):
        row, from_u = order(n)
        even = lax.rem(row, 2) == 0
        return (even, xcopy(n, 2, row, xm1, xr), xcopy(n, 2, row, xp1, xl))

    def stage1(n, first):
        row, from_u = order(n)

        @pl.when(driver)
        def _():
            if first:
                @pl.when(pu < 5)
                def _():
                    zcopy(row, 0, zu).start()

                @pl.when(pd < 5)
                def _():
                    zcopy(row, 8, zd).start()
            else:
                arrived(row, x)

                @pl.when(jnp.logical_and(from_u, pu < 5))
                def _():
                    zcopy(row, n, zu).start()

                @pl.when(jnp.logical_and(jnp.logical_not(from_u), pd < 5))
                def _():
                    zcopy(row, n, zd).start()
            xcopy(n, 0, row, x, xr).start()
            xcopy(n, 1, row, x, xl).start()
            dcopy(row, x).start()

    def stage2(n):
        row, _ = order(n)

        @pl.when(driver)
        def _():
            even, right, left = fwd_copies(n)
            arrived(row, xm1)

            @pl.when(even)
            def _():
                right.start()
            dcopy(row, xm1).start()
            arrived(row, xp1)

            @pl.when(jnp.logical_not(even))
            def _():
                left.start()
            dcopy(row, xp1).start()

    def stage3(n):
        row, _ = order(n)

        @pl.when(driver)
        def _():
            arrived(row, xp2)
            dcopy(row, xp2).start()

        @pl.when(foreign)
        def _():
            for col in range(NX):
                arrived(row, col)

    own_down = remote(tr.at[0], kv.at[r, x], zs_sem.at[0], kv_sem.at[r, x], (zd, t))
    own_up = remote(tr.at[0], kv.at[r, x], zs_sem.at[0], kv_sem.at[r, x], (zu, t))
    hop_down = remote(tr.at[0], tr.at[1], zs_sem.at[0], tr_sem, (zd, t))
    hop_up = remote(tr.at[0], tr.at[1], zs_sem.at[0], tr_sem, (zu, t))
    fwd_down = remote(tr.at[1], kv.at[5, x], zs_sem.at[1], kv_sem.at[5, x], (zd, t))
    fwd_up = remote(tr.at[1], kv.at[6, x], zs_sem.at[1], kv_sem.at[6, x], (zu, t))

    q_sib = remote(qv.at[1], qin.at[0], qs_sem.at[0], q_sem.at[0], (s, sib))
    q_par = remote(qv.at[0], qin.at[1], qs_sem.at[0], q_sem.at[1], (part, t))
    q_pas = remote(qv.at[1], qin.at[1], qs_sem.at[1], q_sem.at[1], (part, sib))

    @pl.when(driver)
    def _():
        own_k.wait()
        own_v.wait()
        stage1(0, True)

    @pl.when(foreign)
    def _():
        tr_k.wait()
        tr_v.wait()
        for rr, cp in ((4, own_down), (5, hop_down), (6, hop_up), (7, own_up)):
            @pl.when(r == rr)
            def _():
                cp.start()

    q_lo.wait()
    q_hi.wait()

    @pl.when(driver)
    def _():
        q_sib.start()

    @pl.when(foreign)
    def _():
        q_par.start()
        q_pas.start()
        for rr, cp in ((4, fwd_down), (7, fwd_up)):
            @pl.when(r == rr)
            def _():
                pltpu.make_async_copy(tr.at[1], tr.at[1], tr_sem).wait()
                cp.start()

    acc[...] = jnp.zeros_like(acc)
    mrow[...] = jnp.full_like(mrow, NEG)

    def split(src, a):
        for h in range(4):
            f = src[:, h * HEAD:(h + 1) * HEAD].astype(jnp.float32) * LOG2_SCALE
            hi = f.astype(jnp.bfloat16)
            lo = (f - hi.astype(jnp.float32)).astype(jnp.bfloat16)
            qhl[a, h] = jnp.concatenate([hi, lo], axis=1)

    @pl.when(driver)
    def _():
        split(qv.at[0], 0)

    @pl.when(foreign)
    def _():
        pltpu.make_async_copy(qin.at[0], qin.at[0], q_sem.at[0]).wait()
        split(qin.at[0], 0)

    stage1(1, False)
    stage2(0)
    pltpu.make_async_copy(qin.at[1], qin.at[1], q_sem.at[1]).wait()
    split(qin.at[1], 1)

    def attend(a, row, pair, offset, masked):
        ks = kv[row, pl.ds(2 * pair, 2), 0].reshape(2 * ROWS, HEAD)
        vs = kv[row, pl.ds(2 * pair, 2), 1].reshape(2 * ROWS, HEAD)
        k2 = jnp.concatenate([ks, ks], axis=1)
        v1 = jnp.concatenate([vs, jnp.ones_like(vs)], axis=1)
        if masked:
            qpos = lax.broadcasted_iota(jnp.int32, (ROWS, 2 * ROWS), 0) + offset
            vis = qpos >= lax.broadcasted_iota(jnp.int32, (ROWS, 2 * ROWS), 1)
        qs = [qhl[a, h] for h in range(4)]
        ms = [mrow[a, h] for h in range(4)]

        def scores(h):
            sc = lax.dot_general(qs[h], k2, (((1,), (1,)), ((), ())),
                                 preferred_element_type=jnp.float32)
            return jnp.where(vis, sc, NEG) if masked else sc

        done = []
        cur = scores(0)
        for h in range(4):
            nxt = scores(h + 1) if h < 3 else None
            mn = jnp.maximum(ms[h], jnp.max(cur, axis=1, keepdims=True))
            al = jnp.exp2(ms[h] - mn)
            p = jnp.exp2(cur - jnp.concatenate([mn] * 4, axis=1)).astype(jnp.bfloat16)
            pv = jnp.dot(p, v1, preferred_element_type=jnp.float32)
            done.append((mn, al, pv))
            cur = nxt
        for h in range(4):
            mn, al, pv = done[h]
            mrow[a, h] = mn
            acc[a, h] = acc[a, h] * jnp.concatenate([al, al], axis=1) + pv

    def row_step(n, carry):
        @pl.when(n < NZ - 2)
        def _():
            stage1(n + 2, False)

        @pl.when(n < NZ - 1)
        def _():
            stage2(n + 1)

        stage3(n)
        row, _ = order(n)
        zr = row + ch * (NZ - 1 - 2 * row)

        def sub(i, carry2):
            a = i // 2
            pair = lax.rem(i, 2)
            bq = s + a * (part - s)
            pos = 2 * zr + pair

            @pl.when(pos < bq // 2)
            def _():
                attend(a, row, pair, 0, False)

            @pl.when(pos == bq // 2)
            def _():
                attend(a, row, pair, lax.rem(bq, 2) * ROWS, True)
            return carry2

        lax.fori_loop(0, 4, sub, 0)
        return carry

    lax.fori_loop(0, NZ, row_step, 0)

    for h in range(4):
        both = jnp.maximum(mrow[0, h], mrow[1, h])
        hm_ref[pl.ds(h, 1), :] = jnp.max(both, axis=0, keepdims=True) * math.log(2.0)
    hm_ref[pl.ds(4, 4), :] = jnp.zeros((4, 128), jnp.float32)

    for a in (1, 0):
        for h in range(4):
            res[a, :, pl.ds(h * HEAD, HEAD)] = (
                acc[a, h, :, :HEAD] / acc[a, h, :, HEAD:]).astype(jnp.bfloat16)

    lo_cols = o_hbm.at[:, pl.ds(0, 512)]
    hi_cols = o_hbm.at[:, pl.ds(512, 512)]
    back_d = remote(res.at[1], lo_cols, os_sem.at[1], o_sem.at[0], (part, t))
    back_s = remote(res.at[1], hi_cols, os_sem.at[1], o_sem.at[1], (part, sib))
    keep_d = pltpu.make_async_copy(res.at[0], lo_cols, os_sem.at[0])
    keep_s = remote(res.at[0], hi_cols, os_sem.at[0], o_sem.at[1], (s, sib))

    @pl.when(driver)
    def _():
        back_d.start()
        keep_d.start()

    @pl.when(foreign)
    def _():
        back_s.start()
        keep_s.start()

    @pl.when(driver)
    def _():
        @pl.when(pu < 5)
        def _():
            zcopy(r, 0, zu).wait_send()

        @pl.when(pd < 5)
        def _():
            zcopy(r, 8, zd).wait_send()

        def drain(n, carry):
            row, from_u = order(n)

            @pl.when(jnp.logical_and(n > 0, jnp.logical_and(from_u, pu < 5)))
            def _():
                zcopy(row, n, zu).wait_send()

            @pl.when(jnp.logical_and(n > 0, jnp.logical_and(jnp.logical_not(from_u), pd < 5)))
            def _():
                zcopy(row, n, zd).wait_send()
            xcopy(n, 0, row, x, xr).wait_send()
            xcopy(n, 1, row, x, xl).wait_send()
            xcopy(n, 2, row, xm1, xr).wait_send()
            for col in range(NX):
                dcopy(row, col).wait_send()
            return carry

        lax.fori_loop(0, NZ, drain, 0)
        q_sib.wait_send()
        back_d.wait_send()
        keep_d.wait()
        keep_s.wait_recv()

    @pl.when(foreign)
    def _():
        own_down.wait_send()

        @pl.when(jnp.logical_or(r == 4, r == 7))
        def _():
            fwd_down.wait_send()
        q_par.wait_send()
        q_pas.wait_send()
        back_s.wait_send()
        keep_s.wait_send()
        back_d.wait_recv()
        back_s.wait_recv()


def attend_all(q, k, v):
    bf = jnp.bfloat16
    return pl.pallas_call(
        attention_kernel,
        out_shape=(jax.ShapeDtypeStruct((ROWS, 1024), bf),
                   jax.ShapeDtypeStruct((8, 128), jnp.float32)),
        in_specs=[pl.BlockSpec(memory_space=pl.ANY)] * 3,
        out_specs=(pl.BlockSpec(memory_space=pl.ANY),
                   pl.BlockSpec(memory_space=pltpu.VMEM)),
        scratch_shapes=[
            pltpu.VMEM((2, ROWS, 512), bf),
            pltpu.VMEM((NZ, NX, 2, ROWS, HEAD), bf),
            pltpu.VMEM((2, 2, ROWS, HEAD), bf),
            pltpu.VMEM((2, ROWS, 512), bf),
            pltpu.VMEM((2, 4, ROWS, 256), bf),
            pltpu.VMEM((2, 4, ROWS, 256), jnp.float32),
            pltpu.VMEM((2, 4, ROWS, 128), jnp.float32),
            pltpu.VMEM((2, ROWS, 512), bf),
            pltpu.SemaphoreType.DMA((4,)),
            pltpu.SemaphoreType.DMA((NZ, NX)),
            pltpu.SemaphoreType.DMA,
            pltpu.SemaphoreType.DMA((2,)),
            pltpu.SemaphoreType.DMA((2,)),
            pltpu.SemaphoreType.DMA((9,)),
            pltpu.SemaphoreType.DMA((NZ, 3)),
            pltpu.SemaphoreType.DMA((NZ, NX)),
            pltpu.SemaphoreType.DMA((2,)),
            pltpu.SemaphoreType.DMA((2,)),
        ],
        compiler_params=pltpu.CompilerParams(
            collective_id=0, has_side_effects=True, vmem_limit_bytes=48 * 2**20),
        name="attend",
    )(q, k, v)


def shards(q, k, v, w, kw):
    heads, groups, per = 64, 8, 8
    s = lax.axis_index("seq")
    t = lax.axis_index("tp")
    out, hm = attend_all(q, k, v)
    ch = s // 16
    c = t % 2
    base = (t - c + ch) * per + 4 * (c != ch).astype(jnp.int32)
    vec = lax.dynamic_update_slice(jnp.full((heads,), -3e38, jnp.float32), hm[:4, 0], (base,))
    head_max = lax.pmax(vec, ("seq", "tp"))
    clip = TAU / jnp.maximum(head_max.reshape(groups, per).max(1), TAU)
    own_max = lax.dynamic_slice(head_max, (t * per,), (per,))
    own_clip = lax.dynamic_slice(clip, (t,), (1,))
    factor = (TAU / jnp.maximum(own_max, TAU)) / jnp.sqrt(own_clip)
    w_out = (w.astype(jnp.float32) * jnp.repeat(factor, HEAD)[None, :]).astype(jnp.bfloat16)
    k_out = (kw.astype(jnp.float32) * jnp.repeat(jnp.sqrt(clip), HEAD)[None, :]).astype(jnp.bfloat16)
    return out, own_max, w_out, k_out


def solution(mesh):
    in_specs = (P("seq", "tp"), P("seq", "tp"), P("seq", "tp"), P("seq", "tp"), P("seq", None))
    out_specs = (P("seq", "tp"), P("tp"), P("seq", "tp"), P("seq", None))
    return jax.shard_map(shards, mesh=mesh, in_specs=in_specs, out_specs=out_specs, check_vma=False)
```

```python
import math

import jax
import jax.numpy as jnp
from jax import lax
from jax.experimental import pallas as pl
from jax.experimental.pallas import tpu as pltpu
from jax.sharding import PartitionSpec as P

HEAD = 128
ROWS = 256
NZ, NX = 8, 4
TAU = 10.0
NEG = -1e30
LOG2_SCALE = math.log2(math.e) / math.sqrt(128.0)
MESH = pl.DeviceIdType.MESH


def attention_kernel(q_hbm, k_hbm, v_hbm, o_hbm, hm_ref,
                     qv, kv, tr, qin, qhl, acc, mrow, res,
                     ld_sem, kv_sem, tr_sem, q_sem, o_sem,
                     zs_sem, xs_sem, ds_sem, qs_sem, os_sem,
                     mx_out, mx_in, ms_sem, mr_sem):
    s = lax.axis_index("seq")
    t = lax.axis_index("tp")
    z = s // NX
    x = lax.rem(s, NX)
    c = lax.rem(t, 2)
    ch = z // (NZ // 2)
    driver = c == ch
    foreign = c != ch
    r = z + c * (NZ - 1 - 2 * z)
    rh = z + ch * (NZ - 1 - 2 * z)
    sib = t + 1 - 2 * c
    part = (NZ - 1 - z) * NX + (NX - 1 - x)
    xr = z * NX + lax.rem(x + 1, NX)
    xl = z * NX + lax.rem(x + NX - 1, NX)
    zu_z = lax.rem(z + NZ + 1 - 2 * c, NZ)
    zd_z = lax.rem(z + NZ - 1 + 2 * c, NZ)
    zu = zu_z * NX + x
    zd = zd_z * NX + x
    pu = lax.rem(r + 2, NZ)
    pd = lax.rem(NZ + 5 - r, NZ)

    own_k = pltpu.make_async_copy(k_hbm, kv.at[r, x, 0], ld_sem.at[0])
    own_v = pltpu.make_async_copy(v_hbm, kv.at[r, x, 1], ld_sem.at[1])
    tr_k = pltpu.make_async_copy(k_hbm, tr.at[0, 0], ld_sem.at[0])
    tr_v = pltpu.make_async_copy(v_hbm, tr.at[0, 1], ld_sem.at[1])
    q_lo = pltpu.make_async_copy(q_hbm.at[:, pl.ds(0, 512)], qv.at[0], ld_sem.at[2])
    q_hi = pltpu.make_async_copy(q_hbm.at[:, pl.ds(512, 512)], qv.at[1], ld_sem.at[3])

    @pl.when(driver)
    def _():
        own_k.start()
        own_v.start()

    @pl.when(foreign)
    def _():
        tr_k.start()
        tr_v.start()

    q_lo.start()
    q_hi.start()

    barrier = pltpu.get_barrier_semaphore()
    row_peers, ring_peers, y_peers = [(s, sib)], [], []
    for d in range(1, NX):
        at = z * NX + lax.rem(x + d, NX)
        row_peers += [(at, t), (at, sib)]
    for d in range(1, NZ):
        ring_peers.append((lax.rem(z + d, NZ) * NX + x, t))
    for d in range(1, 4):
        y_peers.append((s, lax.rem(t + 2 * d, 8)))
    everyone = row_peers + ring_peers + y_peers + [(part, t), (part, sib)]
    for dev in everyone:
        pl.semaphore_signal(barrier, inc=1, device_id=dev, device_id_type=MESH)
    pl.semaphore_wait(barrier, len(everyone))

    def remote(src, dst, send, recv, dev):
        return pltpu.make_async_remote_copy(
            src_ref=src, dst_ref=dst, send_sem=send, recv_sem=recv,
            device_id=dev, device_id_type=MESH)

    def blk(row, col):
        return kv.at[row, col]

    def zcopy(row, slot, dev):
        return remote(blk(row, x), blk(row, x), zs_sem.at[slot], kv_sem.at[row, x], (dev, t))

    def xcopy(n, j, row, col, dev):
        return remote(blk(row, col), blk(row, col), xs_sem.at[n, j], kv_sem.at[row, col], (dev, t))

    def dcopy(row, col):
        return remote(blk(row, col), blk(row, col), ds_sem.at[row, col], kv_sem.at[row, col], (s, sib))

    def arrived(row, col):
        pltpu.make_async_copy(blk(row, col), blk(row, col), kv_sem.at[row, col]).wait()

    def order(n):
        nu = rh + 2
        nd = 5 - rh
        m = jnp.minimum(nu, nd)
        k2 = (n + 1) // 2 - 1
        early = n <= 2 * m
        k = jnp.where(early, k2, n - 1 - m)
        from_u = jnp.where(early, lax.rem(n, 2), (nu > nd).astype(jnp.int32)) == 1
        row = jnp.where(from_u, rh + NZ - 1 - k, rh + 1 + k)
        row = jnp.where(n == 0, rh, lax.rem(row, NZ))
        return row, from_u

    xm1 = lax.rem(x + NX - 1, NX)
    xp1 = lax.rem(x + 1, NX)
    xp2 = lax.rem(x + 2, NX)

    def fwd_copies(n):
        row, from_u = order(n)
        even = lax.rem(row, 2) == 0
        return (even, xcopy(n, 2, row, xm1, xr), xcopy(n, 2, row, xp1, xl))

    def stage1(n, first):
        row, from_u = order(n)

        @pl.when(driver)
        def _():
            if first:
                @pl.when(pu < 5)
                def _():
                    zcopy(row, 0, zu).start()

                @pl.when(pd < 5)
                def _():
                    zcopy(row, 8, zd).start()
            else:
                arrived(row, x)

                @pl.when(jnp.logical_and(from_u, pu < 5))
                def _():
                    zcopy(row, n, zu).start()

                @pl.when(jnp.logical_and(jnp.logical_not(from_u), pd < 5))
                def _():
                    zcopy(row, n, zd).start()
            xcopy(n, 0, row, x, xr).start()
            xcopy(n, 1, row, x, xl).start()
            dcopy(row, x).start()

    def stage2(n):
        row, _ = order(n)

        @pl.when(driver)
        def _():
            even, right, left = fwd_copies(n)
            arrived(row, xm1)

            @pl.when(even)
            def _():
                right.start()
            dcopy(row, xm1).start()
            arrived(row, xp1)

            @pl.when(jnp.logical_not(even))
            def _():
                left.start()
            dcopy(row, xp1).start()

    def stage3(n):
        row, _ = order(n)

        @pl.when(driver)
        def _():
            arrived(row, xp2)
            dcopy(row, xp2).start()

        @pl.when(foreign)
        def _():
            for col in range(NX):
                arrived(row, col)

    own_down = remote(tr.at[0], kv.at[r, x], zs_sem.at[0], kv_sem.at[r, x], (zd, t))
    own_up = remote(tr.at[0], kv.at[r, x], zs_sem.at[0], kv_sem.at[r, x], (zu, t))
    hop_down = remote(tr.at[0], tr.at[1], zs_sem.at[0], tr_sem, (zd, t))
    hop_up = remote(tr.at[0], tr.at[1], zs_sem.at[0], tr_sem, (zu, t))
    fwd_down = remote(tr.at[1], kv.at[5, x], zs_sem.at[1], kv_sem.at[5, x], (zd, t))
    fwd_up = remote(tr.at[1], kv.at[6, x], zs_sem.at[1], kv_sem.at[6, x], (zu, t))

    q_sib = remote(qv.at[1], qin.at[0], qs_sem.at[0], q_sem.at[0], (s, sib))
    q_par = remote(qv.at[0], qin.at[1], qs_sem.at[0], q_sem.at[1], (part, t))
    q_pas = remote(qv.at[1], qin.at[1], qs_sem.at[1], q_sem.at[1], (part, sib))

    @pl.when(driver)
    def _():
        own_k.wait()
        own_v.wait()
        stage1(0, True)

    @pl.when(foreign)
    def _():
        tr_k.wait()
        tr_v.wait()
        for rr, cp in ((4, own_down), (5, hop_down), (6, hop_up), (7, own_up)):
            @pl.when(r == rr)
            def _():
                cp.start()

    q_lo.wait()
    q_hi.wait()

    @pl.when(driver)
    def _():
        q_sib.start()

    @pl.when(foreign)
    def _():
        q_par.start()
        q_pas.start()
        for rr, cp in ((4, fwd_down), (7, fwd_up)):
            @pl.when(r == rr)
            def _():
                pltpu.make_async_copy(tr.at[1], tr.at[1], tr_sem).wait()
                cp.start()

    acc[...] = jnp.zeros_like(acc)
    mrow[...] = jnp.full_like(mrow, NEG)

    def split(src, a):
        for h in range(4):
            f = src[:, h * HEAD:(h + 1) * HEAD].astype(jnp.float32) * LOG2_SCALE
            hi = f.astype(jnp.bfloat16)
            lo = (f - hi.astype(jnp.float32)).astype(jnp.bfloat16)
            qhl[a, h] = jnp.concatenate([hi, lo], axis=1)

    @pl.when(driver)
    def _():
        split(qv.at[0], 0)

    @pl.when(foreign)
    def _():
        pltpu.make_async_copy(qin.at[0], qin.at[0], q_sem.at[0]).wait()
        split(qin.at[0], 0)

    stage1(1, False)
    stage2(0)
    pltpu.make_async_copy(qin.at[1], qin.at[1], q_sem.at[1]).wait()
    split(qin.at[1], 1)

    def attend(a, row, pair, offset, masked):
        ks = kv[row, pl.ds(2 * pair, 2), 0].reshape(2 * ROWS, HEAD)
        vs = kv[row, pl.ds(2 * pair, 2), 1].reshape(2 * ROWS, HEAD)
        k2 = jnp.concatenate([ks, ks], axis=1)
        v1 = jnp.concatenate([vs, jnp.ones_like(vs)], axis=1)
        if masked:
            qpos = lax.broadcasted_iota(jnp.int32, (ROWS, 2 * ROWS), 0) + offset
            vis = qpos >= lax.broadcasted_iota(jnp.int32, (ROWS, 2 * ROWS), 1)
        qs = [qhl[a, h] for h in range(4)]
        ms = [mrow[a, h] for h in range(4)]

        def scores(h):
            sc = lax.dot_general(qs[h], k2, (((1,), (1,)), ((), ())),
                                 preferred_element_type=jnp.float32)
            return jnp.where(vis, sc, NEG) if masked else sc

        done = []
        cur = scores(0)
        for h in range(4):
            nxt = scores(h + 1) if h < 3 else None
            mn = jnp.maximum(ms[h], jnp.max(cur, axis=1, keepdims=True))
            al = jnp.exp2(ms[h] - mn)
            p = jnp.exp2(cur - jnp.concatenate([mn] * 4, axis=1)).astype(jnp.bfloat16)
            pv = jnp.dot(p, v1, preferred_element_type=jnp.float32)
            done.append((mn, al, pv))
            cur = nxt
        for h in range(4):
            mn, al, pv = done[h]
            mrow[a, h] = mn
            acc[a, h] = acc[a, h] * jnp.concatenate([al, al], axis=1) + pv

    def row_step(n, carry):
        @pl.when(n < NZ - 2)
        def _():
            stage1(n + 2, False)

        @pl.when(n < NZ - 1)
        def _():
            stage2(n + 1)

        stage3(n)
        row, _ = order(n)
        zr = row + ch * (NZ - 1 - 2 * row)

        def sub(i, carry2):
            a = i // 2
            pair = lax.rem(i, 2)
            bq = s + a * (part - s)
            pos = 2 * zr + pair

            @pl.when(pos < bq // 2)
            def _():
                attend(a, row, pair, 0, False)

            @pl.when(pos == bq // 2)
            def _():
                attend(a, row, pair, lax.rem(bq, 2) * ROWS, True)
            return carry2

        lax.fori_loop(0, 4, sub, 0)
        return carry

    lax.fori_loop(0, NZ, row_step, 0)

    lane = lax.broadcasted_iota(jnp.int32, (8, 128), 1)
    base = (t - c + ch) * 8 + 4 * (1 - (c == ch).astype(jnp.int32))
    best = jnp.full((8, 128), -3e38, jnp.float32)
    for h in range(4):
        both = jnp.maximum(mrow[0, h], mrow[1, h])
        top = jnp.max(both, axis=0, keepdims=True) * math.log(2.0)
        best = jnp.where(lane == base + h, jnp.broadcast_to(top, (8, 128)), best)
    mx_out[0] = best

    for a in (1, 0):
        for h in range(4):
            res[a, :, pl.ds(h * HEAD, HEAD)] = (
                acc[a, h, :, :HEAD] / acc[a, h, :, HEAD:]).astype(jnp.bfloat16)

    lo_cols = o_hbm.at[:, pl.ds(0, 512)]
    hi_cols = o_hbm.at[:, pl.ds(512, 512)]
    back_d = remote(res.at[1], lo_cols, os_sem.at[1], o_sem.at[0], (part, t))
    back_s = remote(res.at[1], hi_cols, os_sem.at[1], o_sem.at[1], (part, sib))
    keep_d = pltpu.make_async_copy(res.at[0], lo_cols, os_sem.at[0])
    keep_s = remote(res.at[0], hi_cols, os_sem.at[0], o_sem.at[1], (s, sib))

    @pl.when(driver)
    def _():
        back_d.start()
        keep_d.start()

    @pl.when(foreign)
    def _():
        back_s.start()
        keep_s.start()

    at = 0
    for rnd, peers in enumerate((row_peers, ring_peers, y_peers)):
        sends = [remote(mx_out.at[rnd], mx_in.at[at + i], ms_sem.at[at + i], mr_sem.at[at + i], dev)
                 for i, dev in enumerate(peers)]
        for cp in sends:
            cp.start()
        best = mx_out[rnd]
        for i, cp in enumerate(sends):
            cp.wait_recv()
            best = jnp.maximum(best, mx_in[at + i])
        if rnd < 2:
            mx_out[rnd + 1] = best
        at += len(peers)
    for i in range(at):
        remote(mx_out.at[0], mx_in.at[i], ms_sem.at[i], mr_sem.at[i], (s, sib)).wait_send()
    hm_ref[...] = jnp.broadcast_to(best[0:1], (128, 128)).T

    @pl.when(driver)
    def _():
        @pl.when(pu < 5)
        def _():
            zcopy(r, 0, zu).wait_send()

        @pl.when(pd < 5)
        def _():
            zcopy(r, 8, zd).wait_send()

        def drain(n, carry):
            row, from_u = order(n)

            @pl.when(jnp.logical_and(n > 0, jnp.logical_and(from_u, pu < 5)))
            def _():
                zcopy(row, n, zu).wait_send()

            @pl.when(jnp.logical_and(n > 0, jnp.logical_and(jnp.logical_not(from_u), pd < 5)))
            def _():
                zcopy(row, n, zd).wait_send()
            xcopy(n, 0, row, x, xr).wait_send()
            xcopy(n, 1, row, x, xl).wait_send()
            xcopy(n, 2, row, xm1, xr).wait_send()
            for col in range(NX):
                dcopy(row, col).wait_send()
            return carry

        lax.fori_loop(0, NZ, drain, 0)
        q_sib.wait_send()
        back_d.wait_send()
        keep_d.wait()
        keep_s.wait_recv()

    @pl.when(foreign)
    def _():
        own_down.wait_send()

        @pl.when(jnp.logical_or(r == 4, r == 7))
        def _():
            fwd_down.wait_send()
        q_par.wait_send()
        q_pas.wait_send()
        back_s.wait_send()
        keep_s.wait_send()
        back_d.wait_recv()
        back_s.wait_recv()


def attend_all(q, k, v):
    bf = jnp.bfloat16
    return pl.pallas_call(
        attention_kernel,
        out_shape=(jax.ShapeDtypeStruct((ROWS, 1024), bf),
                   jax.ShapeDtypeStruct((128, 128), jnp.float32)),
        in_specs=[pl.BlockSpec(memory_space=pl.ANY)] * 3,
        out_specs=(pl.BlockSpec(memory_space=pl.ANY),
                   pl.BlockSpec(memory_space=pltpu.VMEM)),
        scratch_shapes=[
            pltpu.VMEM((2, ROWS, 512), bf),
            pltpu.VMEM((NZ, NX, 2, ROWS, HEAD), bf),
            pltpu.VMEM((2, 2, ROWS, HEAD), bf),
            pltpu.VMEM((2, ROWS, 512), bf),
            pltpu.VMEM((2, 4, ROWS, 256), bf),
            pltpu.VMEM((2, 4, ROWS, 256), jnp.float32),
            pltpu.VMEM((2, 4, ROWS, 128), jnp.float32),
            pltpu.VMEM((2, ROWS, 512), bf),
            pltpu.SemaphoreType.DMA((4,)),
            pltpu.SemaphoreType.DMA((NZ, NX)),
            pltpu.SemaphoreType.DMA,
            pltpu.SemaphoreType.DMA((2,)),
            pltpu.SemaphoreType.DMA((2,)),
            pltpu.SemaphoreType.DMA((9,)),
            pltpu.SemaphoreType.DMA((NZ, 3)),
            pltpu.SemaphoreType.DMA((NZ, NX)),
            pltpu.SemaphoreType.DMA((2,)),
            pltpu.SemaphoreType.DMA((2,)),
            pltpu.VMEM((3, 8, 128), jnp.float32),
            pltpu.VMEM((17, 8, 128), jnp.float32),
            pltpu.SemaphoreType.DMA((17,)),
            pltpu.SemaphoreType.DMA((17,)),
        ],
        compiler_params=pltpu.CompilerParams(
            collective_id=0, has_side_effects=True, vmem_limit_bytes=67043328),
        name="attend",
    )(q, k, v)


def scale_kernel(hm_ref, w_ref, kw_ref, wo_ref, ko_ref, top_ref):
    t = lax.axis_index("tp")
    for g in range(8):
        most = jnp.max(hm_ref[pl.ds(8 * g, 8), :], axis=0, keepdims=True)
        f = jnp.sqrt(TAU / jnp.maximum(most, TAU))
        cols = slice(g * HEAD, (g + 1) * HEAD)
        ko_ref[:, cols] = (kw_ref[:, cols].astype(jnp.float32) * f).astype(jnp.bfloat16)
    mine = hm_ref[pl.ds(pl.multiple_of(8 * t, 8), 8), :]
    top_ref[...] = mine
    root = jnp.sqrt(TAU / jnp.maximum(jnp.max(mine, axis=0, keepdims=True), TAU))
    gamma = (TAU / jnp.maximum(mine, TAU)) / root
    for h in range(8):
        cols = slice(h * HEAD, (h + 1) * HEAD)
        wo_ref[:, cols] = (w_ref[:, cols].astype(jnp.float32) * gamma[h:h + 1]).astype(jnp.bfloat16)


def scale(hm, w, kw):
    vm = pl.BlockSpec(memory_space=pltpu.VMEM)
    return pl.pallas_call(
        scale_kernel,
        out_shape=(jax.ShapeDtypeStruct(w.shape, w.dtype),
                   jax.ShapeDtypeStruct(kw.shape, kw.dtype),
                   jax.ShapeDtypeStruct((8, 128), jnp.float32)),
        in_specs=[vm] * 3, out_specs=(vm,) * 3, name="scale",
    )(hm, w, kw)


def shards(q, k, v, w, kw):
    out, hm = attend_all(q, k, v)
    w_out, k_out, top = scale(hm, w, kw)
    return out, top[:, 0], w_out, k_out


def solution(mesh):
    in_specs = (P("seq", "tp"), P("seq", "tp"), P("seq", "tp"), P("seq", "tp"), P("seq", None))
    out_specs = (P("seq", "tp"), P("tp"), P("seq", "tp"), P("seq", None))
    return jax.shard_map(shards, mesh=mesh, in_specs=in_specs, out_specs=out_specs, check_vma=False)
```

```python
import math

import jax
import jax.numpy as jnp
from jax import lax
from jax.experimental import pallas as pl
from jax.experimental.pallas import tpu as pltpu
from jax.sharding import PartitionSpec as P

HEAD = 128
ROWS = 256
NZ, NX = 8, 4
TAU = 10.0
NEG = -1e30
LAG = 3
LEAD1, LEAD2 = 6, 3
LOG2_SCALE = math.log2(math.e) / math.sqrt(128.0)
MESH = pl.DeviceIdType.MESH


def attention_kernel(q_hbm, k_hbm, v_hbm, o_hbm, hm_ref,
                     qv, kv, tr, qin, qhl, acc, mrow, res,
                     ld_sem, kv_sem, tr_sem, q_sem, o_sem,
                     zs_sem, xs_sem, ds_sem, qs_sem, os_sem,
                     mx_out, mx_in, ms_sem, mr_sem):
    s = lax.axis_index("seq")
    t = lax.axis_index("tp")
    z = s // NX
    x = lax.rem(s, NX)
    c = lax.rem(t, 2)
    ch = z // (NZ // 2)
    driver = c == ch
    foreign = c != ch
    r = z + c * (NZ - 1 - 2 * z)
    rh = z + ch * (NZ - 1 - 2 * z)
    sib = t + 1 - 2 * c
    part = (NZ - 1 - z) * NX + x
    xr = z * NX + lax.rem(x + 1, NX)
    xl = z * NX + lax.rem(x + NX - 1, NX)
    zu_z = lax.rem(z + NZ + 1 - 2 * c, NZ)
    zd_z = lax.rem(z + NZ - 1 + 2 * c, NZ)
    zu = zu_z * NX + x
    zd = zd_z * NX + x
    pu = lax.rem(r + 2, NZ)
    pd = lax.rem(NZ + 5 - r, NZ)

    own_k = pltpu.make_async_copy(k_hbm, kv.at[r, x, 0], ld_sem.at[0])
    own_v = pltpu.make_async_copy(v_hbm, kv.at[r, x, 1], ld_sem.at[1])
    tr_k = pltpu.make_async_copy(k_hbm, tr.at[0, 0], ld_sem.at[0])
    tr_v = pltpu.make_async_copy(v_hbm, tr.at[0, 1], ld_sem.at[1])
    q_lo = pltpu.make_async_copy(q_hbm.at[:, pl.ds(0, 512)], qv.at[0], ld_sem.at[2])
    q_hi = pltpu.make_async_copy(q_hbm.at[:, pl.ds(512, 512)], qv.at[1], ld_sem.at[3])

    @pl.when(driver)
    def _():
        own_k.start()
        own_v.start()

    @pl.when(foreign)
    def _():
        tr_k.start()
        tr_v.start()

    q_lo.start()
    q_hi.start()

    barrier = pltpu.get_barrier_semaphore()
    row_peers, ring_peers, y_peers = [(s, sib)], [], []
    for d in range(1, NX):
        at = z * NX + lax.rem(x + d, NX)
        row_peers += [(at, t), (at, sib)]
    for d in range(1, NZ):
        ring_peers.append((lax.rem(z + d, NZ) * NX + x, t))
    for d in range(1, 4):
        y_peers.append((s, lax.rem(t + 2 * d, 8)))
    everyone = row_peers + ring_peers + y_peers + [(part, t), (part, sib)]
    for dev in everyone:
        pl.semaphore_signal(barrier, inc=1, device_id=dev, device_id_type=MESH)
    pl.semaphore_wait(barrier, len(everyone))

    def remote(src, dst, send, recv, dev):
        return pltpu.make_async_remote_copy(
            src_ref=src, dst_ref=dst, send_sem=send, recv_sem=recv,
            device_id=dev, device_id_type=MESH)

    def blk(row, col):
        return kv.at[row, col]

    def zcopy(row, slot, dev):
        return remote(blk(row, x), blk(row, x), zs_sem.at[slot], kv_sem.at[row, x], (dev, t))

    def xcopy(n, j, row, col, dev):
        return remote(blk(row, col), blk(row, col), xs_sem.at[n, j], kv_sem.at[row, col], (dev, t))

    def dcopy(row, col):
        return remote(blk(row, col), blk(row, col), ds_sem.at[row, col], kv_sem.at[row, col], (s, sib))

    def arrived(row, col):
        pltpu.make_async_copy(blk(row, col), blk(row, col), kv_sem.at[row, col]).wait()

    def order(n):
        nu = rh + 2
        nd = 5 - rh
        m = jnp.minimum(nu, nd)
        k2 = (n + 1) // 2 - 1
        early = n <= 2 * m
        k = jnp.where(early, k2, n - 1 - m)
        from_u = jnp.where(early, lax.rem(n, 2), (nu > nd).astype(jnp.int32)) == 1
        row = jnp.where(from_u, rh + NZ - 1 - k, rh + 1 + k)
        row = jnp.where(n == 0, rh, lax.rem(row, NZ))
        return row, from_u

    xm1 = lax.rem(x + NX - 1, NX)
    xp1 = lax.rem(x + 1, NX)
    xp2 = lax.rem(x + 2, NX)

    def fwd_copies(n):
        row, from_u = order(n)
        even = lax.rem(row, 2) == 0
        return (even, xcopy(n, 2, row, xm1, xr), xcopy(n, 2, row, xp1, xl))

    def stage1(n, first):
        row, from_u = order(n)

        @pl.when(driver)
        def _():
            if first:
                @pl.when(pu < 5)
                def _():
                    zcopy(row, 0, zu).start()

                @pl.when(pd < 5)
                def _():
                    zcopy(row, 8, zd).start()
            else:
                arrived(row, x)

                @pl.when(jnp.logical_and(from_u, pu < 5))
                def _():
                    zcopy(row, n, zu).start()

                @pl.when(jnp.logical_and(jnp.logical_not(from_u), pd < 5))
                def _():
                    zcopy(row, n, zd).start()
            xcopy(n, 0, row, x, xr).start()
            xcopy(n, 1, row, x, xl).start()
            dcopy(row, x).start()

    def stage2(n):
        row, _ = order(n)

        @pl.when(driver)
        def _():
            even, right, left = fwd_copies(n)
            arrived(row, xm1)

            @pl.when(even)
            def _():
                right.start()
            dcopy(row, xm1).start()
            arrived(row, xp1)

            @pl.when(jnp.logical_not(even))
            def _():
                left.start()
            dcopy(row, xp1).start()

    def stage3(n):
        row, _ = order(n)

        @pl.when(driver)
        def _():
            arrived(row, xp2)
            dcopy(row, xp2).start()

        @pl.when(foreign)
        def _():
            for col in range(NX):
                arrived(row, col)

    own_down = remote(tr.at[0], kv.at[r, x], zs_sem.at[0], kv_sem.at[r, x], (zd, t))
    own_up = remote(tr.at[0], kv.at[r, x], zs_sem.at[0], kv_sem.at[r, x], (zu, t))
    hop_down = remote(tr.at[0], tr.at[1], zs_sem.at[0], tr_sem, (zd, t))
    hop_up = remote(tr.at[0], tr.at[1], zs_sem.at[0], tr_sem, (zu, t))
    fwd_down = remote(tr.at[1], kv.at[5, x], zs_sem.at[1], kv_sem.at[5, x], (zd, t))
    fwd_up = remote(tr.at[1], kv.at[6, x], zs_sem.at[1], kv_sem.at[6, x], (zu, t))

    q_sib = remote(qv.at[1], qin.at[0], qs_sem.at[0], q_sem.at[0], (s, sib))
    q_par = remote(qv.at[0], qin.at[1], qs_sem.at[0], q_sem.at[1], (part, t))
    q_pas = remote(qv.at[1], qin.at[1], qs_sem.at[1], q_sem.at[1], (part, sib))

    @pl.when(driver)
    def _():
        own_k.wait()
        own_v.wait()
        stage1(0, True)

    @pl.when(foreign)
    def _():
        tr_k.wait()
        tr_v.wait()
        for rr, cp in ((4, own_down), (5, hop_down), (6, hop_up), (7, own_up)):
            @pl.when(r == rr)
            def _():
                cp.start()

    q_lo.wait()
    q_hi.wait()

    @pl.when(driver)
    def _():
        q_sib.start()

    @pl.when(foreign)
    def _():
        for rr, cp in ((4, fwd_down), (7, fwd_up)):
            @pl.when(r == rr)
            def _():
                pltpu.make_async_copy(tr.at[1], tr.at[1], tr_sem).wait()
                cp.start()
        q_par.start()
        q_pas.start()

    acc[...] = jnp.zeros_like(acc)
    mrow[...] = jnp.full_like(mrow, NEG)

    def split(src, a):
        for h in range(4):
            f = src[:, h * HEAD:(h + 1) * HEAD].astype(jnp.float32) * LOG2_SCALE
            hi = f.astype(jnp.bfloat16)
            lo = (f - hi.astype(jnp.float32)).astype(jnp.bfloat16)
            qhl[a, h] = jnp.concatenate([hi, lo], axis=1)

    @pl.when(driver)
    def _():
        split(qv.at[0], 0)

    @pl.when(foreign)
    def _():
        pltpu.make_async_copy(qin.at[0], qin.at[0], q_sem.at[0]).wait()
        split(qin.at[0], 0)

    def early(n, carry):
        stage1(n, False)

        @pl.when(n >= LEAD1 - LEAD2)
        def _():
            stage2(n - (LEAD1 - LEAD2))
        return carry

    lax.fori_loop(1, LEAD1, early, 0)

    def attend(a, row, pair, offset, masked):
        ks = kv[row, pl.ds(2 * pair, 2), 0].reshape(2 * ROWS, HEAD)
        vs = kv[row, pl.ds(2 * pair, 2), 1].reshape(2 * ROWS, HEAD)
        k2 = jnp.concatenate([ks, ks], axis=1)
        v1 = jnp.concatenate([vs, jnp.ones_like(vs)], axis=1)
        if masked:
            qpos = lax.broadcasted_iota(jnp.int32, (2 * ROWS, 2 * ROWS), 0)
            qpos = (qpos & (ROWS - 1)) + offset
            vis = qpos >= lax.broadcasted_iota(jnp.int32, (2 * ROWS, 2 * ROWS), 1)
        qs = [qhl[a, pl.ds(2 * h, 2)].reshape(2 * ROWS, 256) for h in range(2)]
        ms = [mrow[a, pl.ds(2 * h, 2)].reshape(2 * ROWS, 128) for h in range(2)]

        def scores(h):
            sc = lax.dot_general(qs[h], k2, (((1,), (1,)), ((), ())),
                                 preferred_element_type=jnp.float32)
            return jnp.where(vis, sc, NEG) if masked else sc

        done = []
        cur = scores(0)
        for h in range(2):
            nxt = scores(h + 1) if h < 1 else None
            mn = jnp.maximum(ms[h], jnp.max(cur, axis=1, keepdims=True))
            al = jnp.exp2(ms[h] - mn)
            p = jnp.exp2(cur - jnp.concatenate([mn] * 4, axis=1)).astype(jnp.bfloat16)
            pv = jnp.dot(p, v1, preferred_element_type=jnp.float32)
            done.append((mn, al, pv))
            cur = nxt
        for h in range(2):
            mn, al, pv = done[h]
            two = pl.ds(2 * h, 2)
            mrow[a, two] = mn.reshape(2, ROWS, 128)
            old = acc[a, two].reshape(2 * ROWS, 256)
            acc[a, two] = (old * jnp.concatenate([al, al], axis=1) + pv).reshape(2, ROWS, 256)

    def row_step(n, carry):
        @pl.when(n < NZ - LEAD1)
        def _():
            stage1(n + LEAD1, False)

        @pl.when(n < NZ - LEAD2)
        def _():
            stage2(n + LEAD2)

        @pl.when(n < NZ)
        def _():
            stage3(n)

        @pl.when(n == LAG)
        def _():
            pltpu.make_async_copy(qin.at[1], qin.at[1], q_sem.at[1]).wait()
            split(qin.at[1], 1)

        def sub(i, carry2):
            a = i // 2
            pair = lax.rem(i, 2)
            m = n - LAG * a
            live = jnp.logical_and(m >= 0, m < NZ)
            row, _ = order(jnp.clip(m, 0, NZ - 1))
            zr = row + ch * (NZ - 1 - 2 * row)
            bq = s + a * (part - s)
            pos = 2 * zr + pair

            @pl.when(jnp.logical_and(live, pos < bq // 2))
            def _():
                attend(a, row, pair, 0, False)

            @pl.when(jnp.logical_and(live, pos == bq // 2))
            def _():
                attend(a, row, pair, lax.rem(bq, 2) * ROWS, True)
            return carry2

        lax.fori_loop(0, 4, sub, 0)
        return carry

    lax.fori_loop(0, NZ + LAG, row_step, 0)

    lane = lax.broadcasted_iota(jnp.int32, (8, 128), 1)
    base = (t - c + ch) * 8 + 4 * (1 - (c == ch).astype(jnp.int32))
    best = jnp.full((8, 128), -3e38, jnp.float32)
    for h in range(4):
        both = jnp.maximum(mrow[0, h], mrow[1, h])
        top = jnp.max(both, axis=0, keepdims=True) * math.log(2.0)
        best = jnp.where(lane == base + h, jnp.broadcast_to(top, (8, 128)), best)
    mx_out[0] = best

    for a in (1, 0):
        for h in range(4):
            res[a, :, pl.ds(h * HEAD, HEAD)] = (
                acc[a, h, :, :HEAD] / acc[a, h, :, HEAD:]).astype(jnp.bfloat16)

    lo_cols = o_hbm.at[:, pl.ds(0, 512)]
    hi_cols = o_hbm.at[:, pl.ds(512, 512)]
    back_d = remote(res.at[1], lo_cols, os_sem.at[1], o_sem.at[0], (part, t))
    back_s = remote(res.at[1], hi_cols, os_sem.at[1], o_sem.at[1], (part, sib))
    keep_d = pltpu.make_async_copy(res.at[0], lo_cols, os_sem.at[0])
    keep_s = remote(res.at[0], hi_cols, os_sem.at[0], o_sem.at[1], (s, sib))

    @pl.when(driver)
    def _():
        back_d.start()
        keep_d.start()

    @pl.when(foreign)
    def _():
        back_s.start()
        keep_s.start()

    at = 0
    for rnd, peers in enumerate((row_peers, ring_peers, y_peers)):
        sends = [remote(mx_out.at[rnd], mx_in.at[at + i], ms_sem.at[at + i], mr_sem.at[at + i], dev)
                 for i, dev in enumerate(peers)]
        for cp in sends:
            cp.start()
        best = mx_out[rnd]
        for i, cp in enumerate(sends):
            cp.wait_recv()
            best = jnp.maximum(best, mx_in[at + i])
        if rnd < 2:
            mx_out[rnd + 1] = best
        at += len(peers)
    for i in range(at):
        remote(mx_out.at[0], mx_in.at[i], ms_sem.at[i], mr_sem.at[i], (s, sib)).wait_send()
    hm_ref[...] = jnp.broadcast_to(best[0:1], (128, 128)).T

    @pl.when(driver)
    def _():
        @pl.when(pu < 5)
        def _():
            zcopy(r, 0, zu).wait_send()

        @pl.when(pd < 5)
        def _():
            zcopy(r, 8, zd).wait_send()

        def drain(n, carry):
            row, from_u = order(n)

            @pl.when(jnp.logical_and(n > 0, jnp.logical_and(from_u, pu < 5)))
            def _():
                zcopy(row, n, zu).wait_send()

            @pl.when(jnp.logical_and(n > 0, jnp.logical_and(jnp.logical_not(from_u), pd < 5)))
            def _():
                zcopy(row, n, zd).wait_send()
            xcopy(n, 0, row, x, xr).wait_send()
            xcopy(n, 1, row, x, xl).wait_send()
            xcopy(n, 2, row, xm1, xr).wait_send()
            for col in range(NX):
                dcopy(row, col).wait_send()
            return carry

        lax.fori_loop(0, NZ, drain, 0)
        q_sib.wait_send()
        back_d.wait_send()
        keep_d.wait()
        keep_s.wait_recv()

    @pl.when(foreign)
    def _():
        own_down.wait_send()

        @pl.when(jnp.logical_or(r == 4, r == 7))
        def _():
            fwd_down.wait_send()
        q_par.wait_send()
        q_pas.wait_send()
        back_s.wait_send()
        keep_s.wait_send()
        back_d.wait_recv()
        back_s.wait_recv()


def attend_all(q, k, v):
    bf = jnp.bfloat16
    return pl.pallas_call(
        attention_kernel,
        out_shape=(jax.ShapeDtypeStruct((ROWS, 1024), bf),
                   jax.ShapeDtypeStruct((128, 128), jnp.float32)),
        in_specs=[pl.BlockSpec(memory_space=pl.ANY)] * 3,
        out_specs=(pl.BlockSpec(memory_space=pl.ANY),
                   pl.BlockSpec(memory_space=pltpu.VMEM)),
        scratch_shapes=[
            pltpu.VMEM((2, ROWS, 512), bf),
            pltpu.VMEM((NZ, NX, 2, ROWS, HEAD), bf),
            pltpu.VMEM((2, 2, ROWS, HEAD), bf),
            pltpu.VMEM((2, ROWS, 512), bf),
            pltpu.VMEM((2, 4, ROWS, 256), bf),
            pltpu.VMEM((2, 4, ROWS, 256), jnp.float32),
            pltpu.VMEM((2, 4, ROWS, 128), jnp.float32),
            pltpu.VMEM((2, ROWS, 512), bf),
            pltpu.SemaphoreType.DMA((4,)),
            pltpu.SemaphoreType.DMA((NZ, NX)),
            pltpu.SemaphoreType.DMA,
            pltpu.SemaphoreType.DMA((2,)),
            pltpu.SemaphoreType.DMA((2,)),
            pltpu.SemaphoreType.DMA((9,)),
            pltpu.SemaphoreType.DMA((NZ, 3)),
            pltpu.SemaphoreType.DMA((NZ, NX)),
            pltpu.SemaphoreType.DMA((2,)),
            pltpu.SemaphoreType.DMA((2,)),
            pltpu.VMEM((3, 8, 128), jnp.float32),
            pltpu.VMEM((17, 8, 128), jnp.float32),
            pltpu.SemaphoreType.DMA((17,)),
            pltpu.SemaphoreType.DMA((17,)),
        ],
        compiler_params=pltpu.CompilerParams(
            collective_id=0, has_side_effects=True, vmem_limit_bytes=67043328),
        name="attend",
    )(q, k, v)


def scale_kernel(hm_ref, w_ref, kw_ref, wo_ref, ko_ref, top_ref):
    t = lax.axis_index("tp")
    for g in range(8):
        most = jnp.max(hm_ref[pl.ds(8 * g, 8), :], axis=0, keepdims=True)
        f = jnp.sqrt(TAU / jnp.maximum(most, TAU))
        cols = slice(g * HEAD, (g + 1) * HEAD)
        ko_ref[:, cols] = (kw_ref[:, cols].astype(jnp.float32) * f).astype(jnp.bfloat16)
    mine = hm_ref[pl.ds(pl.multiple_of(8 * t, 8), 8), :]
    top_ref[...] = mine
    root = jnp.sqrt(TAU / jnp.maximum(jnp.max(mine, axis=0, keepdims=True), TAU))
    gamma = (TAU / jnp.maximum(mine, TAU)) / root
    for h in range(8):
        cols = slice(h * HEAD, (h + 1) * HEAD)
        wo_ref[:, cols] = (w_ref[:, cols].astype(jnp.float32) * gamma[h:h + 1]).astype(jnp.bfloat16)


def scale(hm, w, kw):
    vm = pl.BlockSpec(memory_space=pltpu.VMEM)
    return pl.pallas_call(
        scale_kernel,
        out_shape=(jax.ShapeDtypeStruct(w.shape, w.dtype),
                   jax.ShapeDtypeStruct(kw.shape, kw.dtype),
                   jax.ShapeDtypeStruct((8, 128), jnp.float32)),
        in_specs=[vm] * 3, out_specs=(vm,) * 3, name="scale",
    )(hm, w, kw)


def shards(q, k, v, w, kw):
    out, hm = attend_all(q, k, v)
    w_out, k_out, top = scale(hm, w, kw)
    return out, top[:, 0], w_out, k_out


def solution(mesh):
    in_specs = (P("seq", "tp"), P("seq", "tp"), P("seq", "tp"), P("seq", "tp"), P("seq", None))
    out_specs = (P("seq", "tp"), P("tp"), P("seq", "tp"), P("seq", None))
    return jax.shard_map(shards, mesh=mesh, in_specs=in_specs, out_specs=out_specs, check_vma=False)
```

```python
import math

import jax
import jax.numpy as jnp
from jax import lax
from jax.experimental import pallas as pl
from jax.experimental.pallas import tpu as pltpu
from jax.sharding import PartitionSpec as P

HEAD = 128
ROWS = 256
NZ, NX = 8, 4
TAU = 10.0
NEG = -1e30
LATE = 3
LEAD1, LEAD2 = 4, 2
LOG2_SCALE = math.log2(math.e) / math.sqrt(128.0)
MESH = pl.DeviceIdType.MESH


def attention_kernel(q_hbm, k_hbm, v_hbm, o_hbm, hm_ref,
                     qv, kv, tr, qin, qhl, acc, mrow, res,
                     ld_sem, kv_sem, tr_sem, q_sem, o_sem,
                     zs_sem, xs_sem, ds_sem, qs_sem, os_sem,
                     mx_out, mx_in, ms_sem, mr_sem):
    s = lax.axis_index("seq")
    t = lax.axis_index("tp")
    z = s // NX
    x = lax.rem(s, NX)
    c = lax.rem(t, 2)
    ch = z // (NZ // 2)
    driver = c == ch
    foreign = c != ch
    r = z + c * (NZ - 1 - 2 * z)
    rh = z + ch * (NZ - 1 - 2 * z)
    sib = t + 1 - 2 * c
    part = (NZ - 1 - z) * NX + x
    xr = z * NX + lax.rem(x + 1, NX)
    xl = z * NX + lax.rem(x + NX - 1, NX)
    zu_z = lax.rem(z + NZ + 1 - 2 * c, NZ)
    zd_z = lax.rem(z + NZ - 1 + 2 * c, NZ)
    zu = zu_z * NX + x
    zd = zd_z * NX + x
    pu = lax.rem(r + 2, NZ)
    pd = lax.rem(NZ + 5 - r, NZ)

    own_k = pltpu.make_async_copy(k_hbm, kv.at[r, x, 0], ld_sem.at[0])
    own_v = pltpu.make_async_copy(v_hbm, kv.at[r, x, 1], ld_sem.at[1])
    tr_k = pltpu.make_async_copy(k_hbm, tr.at[0, 0], ld_sem.at[0])
    tr_v = pltpu.make_async_copy(v_hbm, tr.at[0, 1], ld_sem.at[1])
    q_lo = pltpu.make_async_copy(q_hbm.at[:, pl.ds(0, 512)], qv.at[0], ld_sem.at[2])
    q_hi = pltpu.make_async_copy(q_hbm.at[:, pl.ds(512, 512)], qv.at[1], ld_sem.at[3])

    @pl.when(driver)
    def _():
        own_k.start()
        own_v.start()

    @pl.when(foreign)
    def _():
        tr_k.start()
        tr_v.start()

    q_lo.start()
    q_hi.start()

    barrier = pltpu.get_barrier_semaphore()
    row_peers, ring_peers, y_peers = [(s, sib)], [], []
    for d in range(1, NX):
        at = z * NX + lax.rem(x + d, NX)
        row_peers += [(at, t), (at, sib)]
    for d in range(1, NZ):
        ring_peers.append((lax.rem(z + d, NZ) * NX + x, t))
    for d in range(1, 4):
        y_peers.append((s, lax.rem(t + 2 * d, 8)))
    everyone = row_peers + ring_peers + y_peers + [(part, t), (part, sib)]
    for dev in everyone:
        pl.semaphore_signal(barrier, inc=1, device_id=dev, device_id_type=MESH)
    pl.semaphore_wait(barrier, len(everyone))

    def remote(src, dst, send, recv, dev):
        return pltpu.make_async_remote_copy(
            src_ref=src, dst_ref=dst, send_sem=send, recv_sem=recv,
            device_id=dev, device_id_type=MESH)

    def blk(row, col):
        return kv.at[row, col]

    def zcopy(row, slot, dev):
        return remote(blk(row, x), blk(row, x), zs_sem.at[slot], kv_sem.at[row, x], (dev, t))

    def xcopy(n, j, row, col, dev):
        return remote(blk(row, col), blk(row, col), xs_sem.at[n, j], kv_sem.at[row, col], (dev, t))

    def dcopy(row, col):
        return remote(blk(row, col), blk(row, col), ds_sem.at[row, col], kv_sem.at[row, col], (s, sib))

    def arrived(row, col):
        pltpu.make_async_copy(blk(row, col), blk(row, col), kv_sem.at[row, col]).wait()

    def order(n):
        nu = rh + 2
        nd = 5 - rh
        m = jnp.minimum(nu, nd)
        k2 = (n + 1) // 2 - 1
        early = n <= 2 * m
        k = jnp.where(early, k2, n - 1 - m)
        from_u = jnp.where(early, lax.rem(n, 2), (nu > nd).astype(jnp.int32)) == 1
        row = jnp.where(from_u, rh + NZ - 1 - k, rh + 1 + k)
        row = jnp.where(n == 0, rh, lax.rem(row, NZ))
        return row, from_u

    xm1 = lax.rem(x + NX - 1, NX)
    xp1 = lax.rem(x + 1, NX)
    xp2 = lax.rem(x + 2, NX)

    def fwd_copies(n):
        row, from_u = order(n)
        even = lax.rem(row, 2) == 0
        return (even, xcopy(n, 2, row, xm1, xr), xcopy(n, 2, row, xp1, xl))

    def stage1(n, first):
        row, from_u = order(n)

        @pl.when(driver)
        def _():
            if first:
                @pl.when(pu < 5)
                def _():
                    zcopy(row, 0, zu).start()

                @pl.when(pd < 5)
                def _():
                    zcopy(row, 8, zd).start()
            else:
                arrived(row, x)

                @pl.when(jnp.logical_and(from_u, pu < 5))
                def _():
                    zcopy(row, n, zu).start()

                @pl.when(jnp.logical_and(jnp.logical_not(from_u), pd < 5))
                def _():
                    zcopy(row, n, zd).start()
            xcopy(n, 0, row, x, xr).start()
            xcopy(n, 1, row, x, xl).start()
            dcopy(row, x).start()

    def stage2(n):
        row, _ = order(n)

        @pl.when(driver)
        def _():
            even, right, left = fwd_copies(n)
            arrived(row, xm1)

            @pl.when(even)
            def _():
                right.start()
            dcopy(row, xm1).start()
            arrived(row, xp1)

            @pl.when(jnp.logical_not(even))
            def _():
                left.start()
            dcopy(row, xp1).start()

    def stage3(n):
        row, _ = order(n)

        @pl.when(driver)
        def _():
            arrived(row, xp2)
            dcopy(row, xp2).start()

        @pl.when(foreign)
        def _():
            for col in range(NX):
                arrived(row, col)

    own_down = remote(tr.at[0], kv.at[r, x], zs_sem.at[0], kv_sem.at[r, x], (zd, t))
    own_up = remote(tr.at[0], kv.at[r, x], zs_sem.at[0], kv_sem.at[r, x], (zu, t))
    hop_down = remote(tr.at[0], tr.at[1], zs_sem.at[0], tr_sem, (zd, t))
    hop_up = remote(tr.at[0], tr.at[1], zs_sem.at[0], tr_sem, (zu, t))
    fwd_down = remote(tr.at[1], kv.at[5, x], zs_sem.at[1], kv_sem.at[5, x], (zd, t))
    fwd_up = remote(tr.at[1], kv.at[6, x], zs_sem.at[1], kv_sem.at[6, x], (zu, t))

    q_sib = remote(qv.at[1], qin.at[0], qs_sem.at[0], q_sem.at[0], (s, sib))
    q_par = remote(qv.at[0], qin.at[1], qs_sem.at[0], q_sem.at[1], (part, t))
    q_pas = remote(qv.at[1], qin.at[1], qs_sem.at[1], q_sem.at[1], (part, sib))

    @pl.when(driver)
    def _():
        own_k.wait()
        own_v.wait()
        stage1(0, True)

    @pl.when(foreign)
    def _():
        tr_k.wait()
        tr_v.wait()
        for rr, cp in ((4, own_down), (5, hop_down), (6, hop_up), (7, own_up)):
            @pl.when(r == rr)
            def _():
                cp.start()

    q_lo.wait()
    q_hi.wait()

    @pl.when(driver)
    def _():
        q_sib.start()

    @pl.when(foreign)
    def _():
        for rr, cp in ((4, fwd_down), (7, fwd_up)):
            @pl.when(r == rr)
            def _():
                pltpu.make_async_copy(tr.at[1], tr.at[1], tr_sem).wait()
                cp.start()
        q_par.start()
        q_pas.start()

    acc[...] = jnp.zeros_like(acc)
    mrow[...] = jnp.full_like(mrow, NEG)

    def split(src, a):
        for h in range(4):
            f = src[:, h * HEAD:(h + 1) * HEAD].astype(jnp.float32) * LOG2_SCALE
            hi = f.astype(jnp.bfloat16)
            lo = (f - hi.astype(jnp.float32)).astype(jnp.bfloat16)
            qhl[a, h] = jnp.concatenate([hi, lo], axis=1)

    @pl.when(driver)
    def _():
        split(qv.at[0], 0)

    @pl.when(foreign)
    def _():
        pltpu.make_async_copy(qin.at[0], qin.at[0], q_sem.at[0]).wait()
        split(qin.at[0], 0)

    def early(n, carry):
        stage1(n, False)

        @pl.when(n >= LEAD1 - LEAD2)
        def _():
            stage2(n - (LEAD1 - LEAD2))
        return carry

    lax.fori_loop(1, LEAD1, early, 0)

    def attend(a, row, pair, offset, masked):
        ks = kv[row, pl.ds(2 * pair, 2), 0].reshape(2 * ROWS, HEAD)
        vs = kv[row, pl.ds(2 * pair, 2), 1].reshape(2 * ROWS, HEAD)
        k2 = jnp.concatenate([ks, ks], axis=1)
        v1 = jnp.concatenate([vs, jnp.ones_like(vs)], axis=1)
        if masked:
            qpos = lax.broadcasted_iota(jnp.int32, (2 * ROWS, 2 * ROWS), 0)
            qpos = (qpos & (ROWS - 1)) + offset
            vis = qpos >= lax.broadcasted_iota(jnp.int32, (2 * ROWS, 2 * ROWS), 1)
        qs = [qhl[a, pl.ds(2 * h, 2)].reshape(2 * ROWS, 256) for h in range(2)]
        ms = [mrow[a, pl.ds(2 * h, 2)].reshape(2 * ROWS, 128) for h in range(2)]

        def scores(h):
            sc = lax.dot_general(qs[h], k2, (((1,), (1,)), ((), ())),
                                 preferred_element_type=jnp.float32)
            return jnp.where(vis, sc, NEG) if masked else sc

        done = []
        cur = scores(0)
        for h in range(2):
            nxt = scores(h + 1) if h < 1 else None
            mn = jnp.maximum(ms[h], jnp.max(cur, axis=1, keepdims=True))
            al = jnp.exp2(ms[h] - mn)
            p = jnp.exp2(cur - jnp.concatenate([mn] * 4, axis=1)).astype(jnp.bfloat16)
            pv = jnp.dot(p, v1, preferred_element_type=jnp.float32)
            done.append((mn, al, pv))
            cur = nxt
        for h in range(2):
            mn, al, pv = done[h]
            two = pl.ds(2 * h, 2)
            mrow[a, two] = mn.reshape(2, ROWS, 128)
            old = acc[a, two].reshape(2 * ROWS, 256)
            acc[a, two] = (old * jnp.concatenate([al, al], axis=1) + pv).reshape(2, ROWS, 256)

    def row_step(n, carry):
        @pl.when(n < NZ - LEAD1)
        def _():
            stage1(n + LEAD1, False)

        @pl.when(n < NZ - LEAD2)
        def _():
            stage2(n + LEAD2)

        @pl.when(n < NZ)
        def _():
            stage3(n)

        @pl.when(n == LATE)
        def _():
            pltpu.make_async_copy(qin.at[1], qin.at[1], q_sem.at[1]).wait()
            split(qin.at[1], 1)

        def sub(i, carry2):
            a = (i >= 2).astype(jnp.int32)
            pair = lax.rem(i, 2)
            last = jnp.minimum(n, 2 * (n - LATE) + 1)
            from_row = jnp.maximum(jnp.minimum(n - 1, 2 * (n - LATE) - 1) + 1, 0)
            m = jnp.where(i < 2, n, from_row + i // 2 - 1)
            live = m <= jnp.where(i < 2, n, last)
            row, _ = order(jnp.clip(m, 0, NZ - 1))
            zr = row + ch * (NZ - 1 - 2 * row)
            bq = s + a * (part - s)
            pos = 2 * zr + pair

            @pl.when(jnp.logical_and(live, pos < bq // 2))
            def _():
                attend(a, row, pair, 0, False)

            @pl.when(jnp.logical_and(live, pos == bq // 2))
            def _():
                attend(a, row, pair, lax.rem(bq, 2) * ROWS, True)
            return carry2

        lax.fori_loop(0, 6, sub, 0)
        return carry

    lax.fori_loop(0, NZ, row_step, 0)

    lane = lax.broadcasted_iota(jnp.int32, (8, 128), 1)
    base = (t - c + ch) * 8 + 4 * (1 - (c == ch).astype(jnp.int32))
    best = jnp.full((8, 128), -3e38, jnp.float32)
    for h in range(4):
        both = jnp.maximum(mrow[0, h], mrow[1, h])
        top = jnp.max(both, axis=0, keepdims=True) * math.log(2.0)
        best = jnp.where(lane == base + h, jnp.broadcast_to(top, (8, 128)), best)
    mx_out[0] = best

    for a in (1, 0):
        for h in range(4):
            res[a, :, pl.ds(h * HEAD, HEAD)] = (
                acc[a, h, :, :HEAD] / acc[a, h, :, HEAD:]).astype(jnp.bfloat16)

    lo_cols = o_hbm.at[:, pl.ds(0, 512)]
    hi_cols = o_hbm.at[:, pl.ds(512, 512)]
    back_d = remote(res.at[1], lo_cols, os_sem.at[1], o_sem.at[0], (part, t))
    back_s = remote(res.at[1], hi_cols, os_sem.at[1], o_sem.at[1], (part, sib))
    keep_d = pltpu.make_async_copy(res.at[0], lo_cols, os_sem.at[0])
    keep_s = remote(res.at[0], hi_cols, os_sem.at[0], o_sem.at[1], (s, sib))

    @pl.when(driver)
    def _():
        back_d.start()
        keep_d.start()

    @pl.when(foreign)
    def _():
        back_s.start()
        keep_s.start()

    at = 0
    for rnd, peers in enumerate((row_peers, ring_peers, y_peers)):
        sends = [remote(mx_out.at[rnd], mx_in.at[at + i], ms_sem.at[at + i], mr_sem.at[at + i], dev)
                 for i, dev in enumerate(peers)]
        for cp in sends:
            cp.start()
        best = mx_out[rnd]
        for i, cp in enumerate(sends):
            cp.wait_recv()
            best = jnp.maximum(best, mx_in[at + i])
        if rnd < 2:
            mx_out[rnd + 1] = best
        at += len(peers)
    for i in range(at):
        remote(mx_out.at[0], mx_in.at[i], ms_sem.at[i], mr_sem.at[i], (s, sib)).wait_send()
    hm_ref[...] = jnp.broadcast_to(best[0:1], (128, 128)).T

    @pl.when(driver)
    def _():
        @pl.when(pu < 5)
        def _():
            zcopy(r, 0, zu).wait_send()

        @pl.when(pd < 5)
        def _():
            zcopy(r, 8, zd).wait_send()

        def drain(n, carry):
            row, from_u = order(n)

            @pl.when(jnp.logical_and(n > 0, jnp.logical_and(from_u, pu < 5)))
            def _():
                zcopy(row, n, zu).wait_send()

            @pl.when(jnp.logical_and(n > 0, jnp.logical_and(jnp.logical_not(from_u), pd < 5)))
            def _():
                zcopy(row, n, zd).wait_send()
            xcopy(n, 0, row, x, xr).wait_send()
            xcopy(n, 1, row, x, xl).wait_send()
            xcopy(n, 2, row, xm1, xr).wait_send()
            for col in range(NX):
                dcopy(row, col).wait_send()
            return carry

        lax.fori_loop(0, NZ, drain, 0)
        q_sib.wait_send()
        back_d.wait_send()
        keep_d.wait()
        keep_s.wait_recv()

    @pl.when(foreign)
    def _():
        own_down.wait_send()

        @pl.when(jnp.logical_or(r == 4, r == 7))
        def _():
            fwd_down.wait_send()
        q_par.wait_send()
        q_pas.wait_send()
        back_s.wait_send()
        keep_s.wait_send()
        back_d.wait_recv()
        back_s.wait_recv()


def attend_all(q, k, v):
    bf = jnp.bfloat16
    return pl.pallas_call(
        attention_kernel,
        out_shape=(jax.ShapeDtypeStruct((ROWS, 1024), bf),
                   jax.ShapeDtypeStruct((128, 128), jnp.float32)),
        in_specs=[pl.BlockSpec(memory_space=pl.ANY)] * 3,
        out_specs=(pl.BlockSpec(memory_space=pl.ANY),
                   pl.BlockSpec(memory_space=pltpu.VMEM)),
        scratch_shapes=[
            pltpu.VMEM((2, ROWS, 512), bf),
            pltpu.VMEM((NZ, NX, 2, ROWS, HEAD), bf),
            pltpu.VMEM((2, 2, ROWS, HEAD), bf),
            pltpu.VMEM((2, ROWS, 512), bf),
            pltpu.VMEM((2, 4, ROWS, 256), bf),
            pltpu.VMEM((2, 4, ROWS, 256), jnp.float32),
            pltpu.VMEM((2, 4, ROWS, 128), jnp.float32),
            pltpu.VMEM((2, ROWS, 512), bf),
            pltpu.SemaphoreType.DMA((4,)),
            pltpu.SemaphoreType.DMA((NZ, NX)),
            pltpu.SemaphoreType.DMA,
            pltpu.SemaphoreType.DMA((2,)),
            pltpu.SemaphoreType.DMA((2,)),
            pltpu.SemaphoreType.DMA((9,)),
            pltpu.SemaphoreType.DMA((NZ, 3)),
            pltpu.SemaphoreType.DMA((NZ, NX)),
            pltpu.SemaphoreType.DMA((2,)),
            pltpu.SemaphoreType.DMA((2,)),
            pltpu.VMEM((3, 8, 128), jnp.float32),
            pltpu.VMEM((17, 8, 128), jnp.float32),
            pltpu.SemaphoreType.DMA((17,)),
            pltpu.SemaphoreType.DMA((17,)),
        ],
        compiler_params=pltpu.CompilerParams(
            collective_id=0, has_side_effects=True, vmem_limit_bytes=67043328),
        name="attend",
    )(q, k, v)


def scale_kernel(hm_ref, w_hbm, kw_hbm, att_hbm, wo_hbm, ko_hbm, ao_hbm, top_ref,
                 w_v, kw_v, att_v, in_sem, out_sem):
    t = lax.axis_index("tp")
    loads = [pltpu.make_async_copy(src, dst, in_sem.at[i]) for i, (src, dst) in enumerate(
        ((kw_hbm, kw_v), (w_hbm, w_v), (att_hbm, att_v)))]
    stores = [pltpu.make_async_copy(src, dst, out_sem.at[i]) for i, (src, dst) in enumerate(
        ((kw_v, ko_hbm), (w_v, wo_hbm), (att_v, ao_hbm)))]
    for cp in loads:
        cp.start()
    mine = hm_ref[pl.ds(pl.multiple_of(8 * t, 8), 8), :]
    root = jnp.sqrt(TAU / jnp.maximum(jnp.max(mine, axis=0, keepdims=True), TAU))
    gamma = (TAU / jnp.maximum(mine, TAU)) / root
    clips = []
    for g in range(8):
        most = jnp.max(hm_ref[pl.ds(8 * g, 8), :], axis=0, keepdims=True)
        clips.append(jnp.sqrt(TAU / jnp.maximum(most, TAU)))
    loads[0].wait()
    for g in range(8):
        cols = slice(g * HEAD, (g + 1) * HEAD)
        kw_v[:, cols] = (kw_v[:, cols].astype(jnp.float32) * clips[g]).astype(jnp.bfloat16)
    stores[0].start()
    loads[1].wait()
    for h in range(8):
        cols = slice(h * HEAD, (h + 1) * HEAD)
        w_v[:, cols] = (w_v[:, cols].astype(jnp.float32) * gamma[h:h + 1]).astype(jnp.bfloat16)
    stores[1].start()
    loads[2].wait()
    stores[2].start()
    lane = lax.broadcasted_iota(jnp.int32, (1, 128), 1)
    row = jnp.zeros((1, 128), jnp.float32)
    for h in range(8):
        row = jnp.where(lane == h, mine[h:h + 1, :], row)
    top_ref[...] = row[:, :8]
    for cp in stores:
        cp.wait()


def scale(hm, w, kw, att):
    vm = pl.BlockSpec(memory_space=pltpu.VMEM)
    hbm = pl.BlockSpec(memory_space=pl.ANY)
    full = jax.ShapeDtypeStruct(w.shape, w.dtype)
    return pl.pallas_call(
        scale_kernel,
        out_shape=(full, full, full, jax.ShapeDtypeStruct((1, 8), jnp.float32)),
        in_specs=[vm, hbm, hbm, hbm], out_specs=(hbm, hbm, hbm, vm),
        scratch_shapes=[pltpu.VMEM(w.shape, w.dtype)] * 3 + [pltpu.SemaphoreType.DMA((3,))] * 2,
        compiler_params=pltpu.CompilerParams(vmem_limit_bytes=67043328),
        name="scale",
    )(hm, w, kw, att)


def shards(q, k, v, w, kw):
    out, hm = attend_all(q, k, v)
    w_out, k_out, att, top = scale(hm, w, kw, out)
    return att, top.reshape(8), w_out, k_out


def solution(mesh):
    in_specs = (P("seq", "tp"), P("seq", "tp"), P("seq", "tp"), P("seq", "tp"), P("seq", None))
    out_specs = (P("seq", "tp"), P("tp"), P("seq", "tp"), P("seq", None))
    return jax.shard_map(shards, mesh=mesh, in_specs=in_specs, out_specs=out_specs, check_vma=False)
```

```python
import math

import jax
import jax.numpy as jnp
from jax import lax
from jax.experimental import pallas as pl
from jax.experimental.pallas import tpu as pltpu
from jax.sharding import PartitionSpec as P

HEAD = 128
ROWS = 256
NZ, NX = 8, 4
TAU = 10.0
NEG = -1e30
LATE = 2
LEAD1, LEAD2 = 4, 2
LOG2_SCALE = math.log2(math.e) / math.sqrt(128.0)
MESH = pl.DeviceIdType.MESH


def attention_kernel(q_hbm, k_hbm, v_hbm, o_hbm, hm_ref,
                     qv, kv, tr, qin, qhl, acc, mrow, res,
                     ld_sem, kv_sem, tr_sem, q_sem, o_sem,
                     zs_sem, xs_sem, ds_sem, qs_sem, os_sem,
                     mx_out, mx_in, ms_sem, mr_sem):
    s = lax.axis_index("seq")
    t = lax.axis_index("tp")
    z = s // NX
    x = lax.rem(s, NX)
    c = lax.rem(t, 2)
    ch = z // (NZ // 2)
    driver = c == ch
    foreign = c != ch
    r = z + c * (NZ - 1 - 2 * z)
    rh = z + ch * (NZ - 1 - 2 * z)
    sib = t + 1 - 2 * c
    part = (NZ - 1 - z) * NX + x
    xr = z * NX + lax.rem(x + 1, NX)
    xl = z * NX + lax.rem(x + NX - 1, NX)
    zu_z = lax.rem(z + NZ + 1 - 2 * c, NZ)
    zd_z = lax.rem(z + NZ - 1 + 2 * c, NZ)
    zu = zu_z * NX + x
    zd = zd_z * NX + x
    pu = lax.rem(r + 2, NZ)
    pd = lax.rem(NZ + 5 - r, NZ)

    own_k = pltpu.make_async_copy(k_hbm, kv.at[r, x, 0], ld_sem.at[0])
    own_v = pltpu.make_async_copy(v_hbm, kv.at[r, x, 1], ld_sem.at[1])
    tr_k = pltpu.make_async_copy(k_hbm, tr.at[0, 0], ld_sem.at[0])
    tr_v = pltpu.make_async_copy(v_hbm, tr.at[0, 1], ld_sem.at[1])
    q_lo = pltpu.make_async_copy(q_hbm.at[:, pl.ds(0, 512)], qv.at[0], ld_sem.at[2])
    q_hi = pltpu.make_async_copy(q_hbm.at[:, pl.ds(512, 512)], qv.at[1], ld_sem.at[3])

    @pl.when(driver)
    def _():
        own_k.start()
        own_v.start()

    @pl.when(foreign)
    def _():
        tr_k.start()
        tr_v.start()

    q_lo.start()
    q_hi.start()

    barrier = pltpu.get_barrier_semaphore()
    row_peers, ring_peers, y_peers = [(s, sib)], [], []
    for d in range(1, NX):
        at = z * NX + lax.rem(x + d, NX)
        row_peers += [(at, t), (at, sib)]
    for d in range(1, NZ):
        ring_peers.append((lax.rem(z + d, NZ) * NX + x, t))
    for d in range(1, 4):
        y_peers.append((s, lax.rem(t + 2 * d, 8)))
    everyone = row_peers + ring_peers + y_peers + [(part, t), (part, sib)]
    for dev in everyone:
        pl.semaphore_signal(barrier, inc=1, device_id=dev, device_id_type=MESH)
    pl.semaphore_wait(barrier, len(everyone))

    def remote(src, dst, send, recv, dev):
        return pltpu.make_async_remote_copy(
            src_ref=src, dst_ref=dst, send_sem=send, recv_sem=recv,
            device_id=dev, device_id_type=MESH)

    def zcopy(row, slot, dev, j):
        b = kv.at[row, x, j]
        return remote(b, b, zs_sem.at[slot, j], kv_sem.at[row, x, j], (dev, t))

    def xcopy(n, way, row, col, dev, j):
        b = kv.at[row, col, j]
        return remote(b, b, xs_sem.at[n, way, j], kv_sem.at[row, col, j], (dev, t))

    def dcopy(row, col, j):
        b = kv.at[row, col, j]
        return remote(b, b, ds_sem.at[row, col, j], kv_sem.at[row, col, j], (s, sib))

    def arrived(row, col, j):
        b = kv.at[row, col, j]
        pltpu.make_async_copy(b, b, kv_sem.at[row, col, j]).wait()

    def order(n):
        nu = rh + 2
        nd = 5 - rh
        m = jnp.minimum(nu, nd)
        k2 = (n + 1) // 2 - 1
        early = n <= 2 * m
        k = jnp.where(early, k2, n - 1 - m)
        from_u = jnp.where(early, lax.rem(n, 2), (nu > nd).astype(jnp.int32)) == 1
        row = jnp.where(from_u, rh + NZ - 1 - k, rh + 1 + k)
        row = jnp.where(n == 0, rh, lax.rem(row, NZ))
        return row, from_u

    xm1 = lax.rem(x + NX - 1, NX)
    xp1 = lax.rem(x + 1, NX)
    xp2 = lax.rem(x + 2, NX)

    def stage1(n, first):
        row, from_u = order(n)

        @pl.when(driver)
        def _():
            for j in range(2):
                if first:
                    @pl.when(pu < 5)
                    def _():
                        zcopy(row, 0, zu, j).start()

                    @pl.when(pd < 5)
                    def _():
                        zcopy(row, 8, zd, j).start()
                else:
                    arrived(row, x, j)

                    @pl.when(jnp.logical_and(from_u, pu < 5))
                    def _():
                        zcopy(row, n, zu, j).start()

                    @pl.when(jnp.logical_and(jnp.logical_not(from_u), pd < 5))
                    def _():
                        zcopy(row, n, zd, j).start()
                xcopy(n, 0, row, x, xr, j).start()
                xcopy(n, 1, row, x, xl, j).start()
                dcopy(row, x, j).start()

    def stage2(n):
        row, _ = order(n)

        @pl.when(driver)
        def _():
            even = lax.rem(row, 2) == 0
            for j in range(2):
                arrived(row, xm1, j)

                @pl.when(even)
                def _():
                    xcopy(n, 2, row, xm1, xr, j).start()
                dcopy(row, xm1, j).start()
                arrived(row, xp1, j)

                @pl.when(jnp.logical_not(even))
                def _():
                    xcopy(n, 2, row, xp1, xl, j).start()
                dcopy(row, xp1, j).start()

    def stage3(n):
        row, _ = order(n)

        @pl.when(driver)
        def _():
            for j in range(2):
                arrived(row, xp2, j)
                dcopy(row, xp2, j).start()

        @pl.when(foreign)
        def _():
            for col in range(NX):
                for j in range(2):
                    arrived(row, col, j)

    def hop(src, dst, slot, recv, dev):
        return [remote(src.at[j], dst.at[j], zs_sem.at[slot, j], recv.at[j], (dev, t))
                for j in range(2)]

    def land(row):
        return kv.at[row, x], kv_sem.at[row, x]

    own_down = hop(tr.at[0], land(r)[0], 0, land(r)[1], zd)
    own_up = hop(tr.at[0], land(r)[0], 0, land(r)[1], zu)
    hop_down = hop(tr.at[0], tr.at[1], 0, tr_sem, zd)
    hop_up = hop(tr.at[0], tr.at[1], 0, tr_sem, zu)
    fwd_down = hop(tr.at[1], land(5)[0], 1, land(5)[1], zd)
    fwd_up = hop(tr.at[1], land(6)[0], 1, land(6)[1], zu)

    q_sib = remote(qv.at[1], qin.at[0], qs_sem.at[0], q_sem.at[0], (s, sib))
    q_par = remote(qv.at[0], qin.at[1], qs_sem.at[0], q_sem.at[1], (part, t))
    q_pas = remote(qv.at[1], qin.at[1], qs_sem.at[1], q_sem.at[1], (part, sib))

    @pl.when(driver)
    def _():
        own_k.wait()
        own_v.wait()
        stage1(0, True)

    @pl.when(foreign)
    def _():
        tr_k.wait()
        tr_v.wait()
        for rr, cps in ((4, own_down), (5, hop_down), (6, hop_up), (7, own_up)):
            @pl.when(r == rr)
            def _():
                for cp in cps:
                    cp.start()

    q_lo.wait()
    q_hi.wait()

    @pl.when(driver)
    def _():
        q_sib.start()

    @pl.when(foreign)
    def _():
        for rr, cps in ((4, fwd_down), (7, fwd_up)):
            @pl.when(r == rr)
            def _():
                for j, cp in enumerate(cps):
                    b = tr.at[1, j]
                    pltpu.make_async_copy(b, b, tr_sem.at[j]).wait()
                    cp.start()
        q_par.start()
        q_pas.start()

    acc[...] = jnp.zeros_like(acc)
    mrow[...] = jnp.full_like(mrow, NEG)

    def split(src, a):
        for h in range(4):
            f = src[:, h * HEAD:(h + 1) * HEAD].astype(jnp.float32) * LOG2_SCALE
            hi = f.astype(jnp.bfloat16)
            lo = (f - hi.astype(jnp.float32)).astype(jnp.bfloat16)
            qhl[a, h] = jnp.concatenate([hi, lo], axis=1)

    @pl.when(driver)
    def _():
        split(qv.at[0], 0)

    @pl.when(foreign)
    def _():
        pltpu.make_async_copy(qin.at[0], qin.at[0], q_sem.at[0]).wait()
        split(qin.at[0], 0)

    def early(n, carry):
        stage1(n, False)

        @pl.when(n >= LEAD1 - LEAD2)
        def _():
            stage2(n - (LEAD1 - LEAD2))
        return carry

    lax.fori_loop(1, LEAD1, early, 0)

    def attend(a, row, pair, offset, masked):
        ks = kv[row, pl.ds(2 * pair, 2), 0].reshape(2 * ROWS, HEAD)
        vs = kv[row, pl.ds(2 * pair, 2), 1].reshape(2 * ROWS, HEAD)
        k2 = jnp.concatenate([ks, ks], axis=1)
        v1 = jnp.concatenate([vs, jnp.ones_like(vs)], axis=1)
        if masked:
            qpos = lax.broadcasted_iota(jnp.int32, (2 * ROWS, 2 * ROWS), 0)
            qpos = (qpos & (ROWS - 1)) + offset
            vis = qpos >= lax.broadcasted_iota(jnp.int32, (2 * ROWS, 2 * ROWS), 1)
        qs = [qhl[a, pl.ds(2 * h, 2)].reshape(2 * ROWS, 256) for h in range(2)]
        ms = [mrow[a, pl.ds(2 * h, 2)].reshape(2 * ROWS, 128) for h in range(2)]

        def scores(h):
            sc = lax.dot_general(qs[h], k2, (((1,), (1,)), ((), ())),
                                 preferred_element_type=jnp.float32)
            return jnp.where(vis, sc, NEG) if masked else sc

        done = []
        cur = scores(0)
        for h in range(2):
            nxt = scores(h + 1) if h < 1 else None
            mn = jnp.maximum(ms[h], jnp.max(cur, axis=1, keepdims=True))
            al = jnp.exp2(ms[h] - mn)
            p = jnp.exp2(cur - jnp.concatenate([mn] * 4, axis=1)).astype(jnp.bfloat16)
            pv = jnp.dot(p, v1, preferred_element_type=jnp.float32)
            done.append((mn, al, pv))
            cur = nxt
        for h in range(2):
            mn, al, pv = done[h]
            two = pl.ds(2 * h, 2)
            mrow[a, two] = mn.reshape(2, ROWS, 128)
            old = acc[a, two].reshape(2 * ROWS, 256)
            acc[a, two] = (old * jnp.concatenate([al, al], axis=1) + pv).reshape(2, ROWS, 256)

    def row_step(n, carry):
        @pl.when(n < NZ - LEAD1)
        def _():
            stage1(n + LEAD1, False)

        @pl.when(n < NZ - LEAD2)
        def _():
            stage2(n + LEAD2)

        @pl.when(n < NZ)
        def _():
            stage3(n)

        @pl.when(n == LATE)
        def _():
            pltpu.make_async_copy(qin.at[1], qin.at[1], q_sem.at[1]).wait()
            split(qin.at[1], 1)

        def sub(i, carry2):
            a = (i >= 2).astype(jnp.int32)
            pair = lax.rem(i, 2)
            last = jnp.minimum(n, 2 * (n - LATE) + 1)
            from_row = jnp.maximum(jnp.minimum(n - 1, 2 * (n - LATE) - 1) + 1, 0)
            m = jnp.where(i < 2, n, from_row + i // 2 - 1)
            live = m <= jnp.where(i < 2, n, last)
            row, _ = order(jnp.clip(m, 0, NZ - 1))
            zr = row + ch * (NZ - 1 - 2 * row)
            bq = s + a * (part - s)
            pos = 2 * zr + pair

            @pl.when(jnp.logical_and(live, pos < bq // 2))
            def _():
                attend(a, row, pair, 0, False)

            @pl.when(jnp.logical_and(live, pos == bq // 2))
            def _():
                attend(a, row, pair, lax.rem(bq, 2) * ROWS, True)
            return carry2

        lax.fori_loop(0, 6, sub, 0)
        return carry

    lax.fori_loop(0, NZ, row_step, 0)

    lane = lax.broadcasted_iota(jnp.int32, (8, 128), 1)
    base = (t - c + ch) * 8 + 4 * (1 - (c == ch).astype(jnp.int32))
    best = jnp.full((8, 128), -3e38, jnp.float32)
    for h in range(4):
        both = jnp.maximum(mrow[0, h], mrow[1, h])
        top = jnp.max(both, axis=0, keepdims=True) * math.log(2.0)
        best = jnp.where(lane == base + h, jnp.broadcast_to(top, (8, 128)), best)
    mx_out[0] = best

    for a in (1, 0):
        for h in range(4):
            res[a, :, pl.ds(h * HEAD, HEAD)] = (
                acc[a, h, :, :HEAD] / acc[a, h, :, HEAD:]).astype(jnp.bfloat16)

    lo_cols = o_hbm.at[:, pl.ds(0, 512)]
    hi_cols = o_hbm.at[:, pl.ds(512, 512)]
    back_d = remote(res.at[1], lo_cols, os_sem.at[1], o_sem.at[0], (part, t))
    back_s = remote(res.at[1], hi_cols, os_sem.at[1], o_sem.at[1], (part, sib))
    keep_d = pltpu.make_async_copy(res.at[0], lo_cols, os_sem.at[0])
    keep_s = remote(res.at[0], hi_cols, os_sem.at[0], o_sem.at[1], (s, sib))

    @pl.when(driver)
    def _():
        back_d.start()
        keep_d.start()

    @pl.when(foreign)
    def _():
        back_s.start()
        keep_s.start()

    at = 0
    for rnd, peers in enumerate((row_peers, ring_peers, y_peers)):
        sends = [remote(mx_out.at[rnd], mx_in.at[at + i], ms_sem.at[at + i], mr_sem.at[at + i], dev)
                 for i, dev in enumerate(peers)]
        for cp in sends:
            cp.start()
        best = mx_out[rnd]
        for i, cp in enumerate(sends):
            cp.wait_recv()
            best = jnp.maximum(best, mx_in[at + i])
        if rnd < 2:
            mx_out[rnd + 1] = best
        at += len(peers)
    for i in range(at):
        remote(mx_out.at[0], mx_in.at[i], ms_sem.at[i], mr_sem.at[i], (s, sib)).wait_send()
    hm_ref[...] = jnp.broadcast_to(best[0:1], (128, 128)).T

    @pl.when(driver)
    def _():
        for j in range(2):
            @pl.when(pu < 5)
            def _():
                zcopy(r, 0, zu, j).wait_send()

            @pl.when(pd < 5)
            def _():
                zcopy(r, 8, zd, j).wait_send()

        def drain(n, carry):
            row, from_u = order(n)
            for j in range(2):
                @pl.when(jnp.logical_and(n > 0, jnp.logical_and(from_u, pu < 5)))
                def _():
                    zcopy(row, n, zu, j).wait_send()

                @pl.when(jnp.logical_and(n > 0, jnp.logical_and(jnp.logical_not(from_u), pd < 5)))
                def _():
                    zcopy(row, n, zd, j).wait_send()
                xcopy(n, 0, row, x, xr, j).wait_send()
                xcopy(n, 1, row, x, xl, j).wait_send()
                xcopy(n, 2, row, xm1, xr, j).wait_send()
                for col in range(NX):
                    dcopy(row, col, j).wait_send()
            return carry

        lax.fori_loop(0, NZ, drain, 0)
        q_sib.wait_send()
        back_d.wait_send()
        keep_d.wait()
        keep_s.wait_recv()

    @pl.when(foreign)
    def _():
        for cp in own_down:
            cp.wait_send()

        @pl.when(jnp.logical_or(r == 4, r == 7))
        def _():
            for cp in fwd_down:
                cp.wait_send()
        q_par.wait_send()
        q_pas.wait_send()
        back_s.wait_send()
        keep_s.wait_send()
        back_d.wait_recv()
        back_s.wait_recv()


def attend_all(q, k, v):
    bf = jnp.bfloat16
    return pl.pallas_call(
        attention_kernel,
        out_shape=(jax.ShapeDtypeStruct((ROWS, 1024), bf),
                   jax.ShapeDtypeStruct((128, 128), jnp.float32)),
        in_specs=[pl.BlockSpec(memory_space=pl.ANY)] * 3,
        out_specs=(pl.BlockSpec(memory_space=pl.ANY),
                   pl.BlockSpec(memory_space=pltpu.VMEM)),
        scratch_shapes=[
            pltpu.VMEM((2, ROWS, 512), bf),
            pltpu.VMEM((NZ, NX, 2, ROWS, HEAD), bf),
            pltpu.VMEM((2, 2, ROWS, HEAD), bf),
            pltpu.VMEM((2, ROWS, 512), bf),
            pltpu.VMEM((2, 4, ROWS, 256), bf),
            pltpu.VMEM((2, 4, ROWS, 256), jnp.float32),
            pltpu.VMEM((2, 4, ROWS, 128), jnp.float32),
            pltpu.VMEM((2, ROWS, 512), bf),
            pltpu.SemaphoreType.DMA((4,)),
            pltpu.SemaphoreType.DMA((NZ, NX, 2)),
            pltpu.SemaphoreType.DMA((2,)),
            pltpu.SemaphoreType.DMA((2,)),
            pltpu.SemaphoreType.DMA((2,)),
            pltpu.SemaphoreType.DMA((9, 2)),
            pltpu.SemaphoreType.DMA((NZ, 3, 2)),
            pltpu.SemaphoreType.DMA((NZ, NX, 2)),
            pltpu.SemaphoreType.DMA((2,)),
            pltpu.SemaphoreType.DMA((2,)),
            pltpu.VMEM((3, 8, 128), jnp.float32),
            pltpu.VMEM((17, 8, 128), jnp.float32),
            pltpu.SemaphoreType.DMA((17,)),
            pltpu.SemaphoreType.DMA((17,)),
        ],
        compiler_params=pltpu.CompilerParams(
            collective_id=0, has_side_effects=True, vmem_limit_bytes=67043328),
        name="attend",
    )(q, k, v)


def scale_kernel(hm_ref, w_hbm, kw_hbm, att_hbm, wo_hbm, ko_hbm, ao_hbm, top_ref,
                 w_v, kw_v, att_v, in_sem, out_sem):
    t = lax.axis_index("tp")
    loads = [pltpu.make_async_copy(src, dst, in_sem.at[i]) for i, (src, dst) in enumerate(
        ((kw_hbm, kw_v), (w_hbm, w_v), (att_hbm, att_v)))]
    stores = [pltpu.make_async_copy(src, dst, out_sem.at[i]) for i, (src, dst) in enumerate(
        ((kw_v, ko_hbm), (w_v, wo_hbm), (att_v, ao_hbm)))]
    for cp in loads:
        cp.start()
    mine = hm_ref[pl.ds(pl.multiple_of(8 * t, 8), 8), :]
    root = jnp.sqrt(TAU / jnp.maximum(jnp.max(mine, axis=0, keepdims=True), TAU))
    gamma = (TAU / jnp.maximum(mine, TAU)) / root
    clips = []
    for g in range(8):
        most = jnp.max(hm_ref[pl.ds(8 * g, 8), :], axis=0, keepdims=True)
        clips.append(jnp.sqrt(TAU / jnp.maximum(most, TAU)))
    loads[0].wait()
    for g in range(8):
        cols = slice(g * HEAD, (g + 1) * HEAD)
        kw_v[:, cols] = (kw_v[:, cols].astype(jnp.float32) * clips[g]).astype(jnp.bfloat16)
    stores[0].start()
    loads[1].wait()
    for h in range(8):
        cols = slice(h * HEAD, (h + 1) * HEAD)
        w_v[:, cols] = (w_v[:, cols].astype(jnp.float32) * gamma[h:h + 1]).astype(jnp.bfloat16)
    stores[1].start()
    loads[2].wait()
    stores[2].start()
    lane = lax.broadcasted_iota(jnp.int32, (1, 128), 1)
    row = jnp.zeros((1, 128), jnp.float32)
    for h in range(8):
        row = jnp.where(lane == h, mine[h:h + 1, :], row)
    top_ref[...] = row[:, :8]
    for cp in stores:
        cp.wait()


def scale(hm, w, kw, att):
    vm = pl.BlockSpec(memory_space=pltpu.VMEM)
    hbm = pl.BlockSpec(memory_space=pl.ANY)
    full = jax.ShapeDtypeStruct(w.shape, w.dtype)
    return pl.pallas_call(
        scale_kernel,
        out_shape=(full, full, full, jax.ShapeDtypeStruct((1, 8), jnp.float32)),
        in_specs=[vm, hbm, hbm, hbm], out_specs=(hbm, hbm, hbm, vm),
        scratch_shapes=[pltpu.VMEM(w.shape, w.dtype)] * 3 + [pltpu.SemaphoreType.DMA((3,))] * 2,
        compiler_params=pltpu.CompilerParams(vmem_limit_bytes=67043328),
        name="scale",
    )(hm, w, kw, att)


def shards(q, k, v, w, kw):
    out, hm = attend_all(q, k, v)
    w_out, k_out, att, top = scale(hm, w, kw, out)
    return att, top.reshape(8), w_out, k_out


def solution(mesh):
    in_specs = (P("seq", "tp"), P("seq", "tp"), P("seq", "tp"), P("seq", "tp"), P("seq", None))
    out_specs = (P("seq", "tp"), P("tp"), P("seq", "tp"), P("seq", None))
    return jax.shard_map(shards, mesh=mesh, in_specs=in_specs, out_specs=out_specs, check_vma=False)
```

```python
import math

import jax
import jax.numpy as jnp
from jax import lax
from jax.experimental import pallas as pl
from jax.experimental.pallas import tpu as pltpu
from jax.sharding import PartitionSpec as P

HEAD = 128
ROWS = 256
NZ, NX = 8, 4
TAU = 10.0
NEG = -1e30
LATE = 2
LEAD1, LEAD2 = 5, 3
LOG2_SCALE = math.log2(math.e) / math.sqrt(128.0)
MESH = pl.DeviceIdType.MESH


def attention_kernel(q_hbm, k_hbm, v_hbm, o_hbm, hm_ref,
                     qv, kv, tr, qin, qhl, acc, mrow, res,
                     ld_sem, kv_sem, tr_sem, q_sem, o_sem,
                     zs_sem, xs_sem, ds_sem, qs_sem, os_sem,
                     mx_out, mx_in, ms_sem, mr_sem):
    s = lax.axis_index("seq")
    t = lax.axis_index("tp")
    z = s // NX
    x = lax.rem(s, NX)
    c = lax.rem(t, 2)
    ch = z // (NZ // 2)
    driver = c == ch
    foreign = c != ch
    r = z + c * (NZ - 1 - 2 * z)
    rh = z + ch * (NZ - 1 - 2 * z)
    sib = t + 1 - 2 * c
    part = (NZ - 1 - z) * NX + x
    xr = z * NX + lax.rem(x + 1, NX)
    xl = z * NX + lax.rem(x + NX - 1, NX)
    zu_z = lax.rem(z + NZ + 1 - 2 * c, NZ)
    zd_z = lax.rem(z + NZ - 1 + 2 * c, NZ)
    zu = zu_z * NX + x
    zd = zd_z * NX + x
    pu = lax.rem(r + 2, NZ)
    pd = lax.rem(NZ + 5 - r, NZ)

    own_k = pltpu.make_async_copy(k_hbm, kv.at[r, x, 0], ld_sem.at[0])
    own_v = pltpu.make_async_copy(v_hbm, kv.at[r, x, 1], ld_sem.at[1])
    tr_k = pltpu.make_async_copy(k_hbm, tr.at[0, 0], ld_sem.at[0])
    tr_v = pltpu.make_async_copy(v_hbm, tr.at[0, 1], ld_sem.at[1])
    q_lo = pltpu.make_async_copy(q_hbm.at[:, pl.ds(0, 512)], qv.at[0], ld_sem.at[2])
    q_hi = pltpu.make_async_copy(q_hbm.at[:, pl.ds(512, 512)], qv.at[1], ld_sem.at[3])

    @pl.when(driver)
    def _():
        own_k.start()
        own_v.start()

    @pl.when(foreign)
    def _():
        tr_k.start()
        tr_v.start()

    q_lo.start()
    q_hi.start()

    barrier = pltpu.get_barrier_semaphore()
    row_peers, ring_peers, y_peers = [(s, sib)], [], []
    for d in range(1, NX):
        at = z * NX + lax.rem(x + d, NX)
        row_peers += [(at, t), (at, sib)]
    for d in range(1, NZ):
        ring_peers.append((lax.rem(z + d, NZ) * NX + x, t))
    for d in range(1, 4):
        y_peers.append((s, lax.rem(t + 2 * d, 8)))
    everyone = row_peers + ring_peers + y_peers + [(part, t), (part, sib)]
    for dev in everyone:
        pl.semaphore_signal(barrier, inc=1, device_id=dev, device_id_type=MESH)
    pl.semaphore_wait(barrier, len(everyone))

    def remote(src, dst, send, recv, dev):
        return pltpu.make_async_remote_copy(
            src_ref=src, dst_ref=dst, send_sem=send, recv_sem=recv,
            device_id=dev, device_id_type=MESH)

    def zcopy(row, slot, dev, j):
        b = kv.at[row, x, j]
        return remote(b, b, zs_sem.at[slot, j], kv_sem.at[row, x, j], (dev, t))

    def xcopy(n, way, row, col, dev, j):
        b = kv.at[row, col, j]
        return remote(b, b, xs_sem.at[n, way, j], kv_sem.at[row, col, j], (dev, t))

    def dcopy(row, col, j):
        b = kv.at[row, col, j]
        return remote(b, b, ds_sem.at[row, col, j], kv_sem.at[row, col, j], (s, sib))

    def arrived(row, col, j):
        b = kv.at[row, col, j]
        pltpu.make_async_copy(b, b, kv_sem.at[row, col, j]).wait()

    def order(n):
        nu = rh + 2
        nd = 5 - rh
        m = jnp.minimum(nu, nd)
        k2 = (n + 1) // 2 - 1
        early = n <= 2 * m
        k = jnp.where(early, k2, n - 1 - m)
        from_u = jnp.where(early, lax.rem(n, 2), (nu > nd).astype(jnp.int32)) == 1
        row = jnp.where(from_u, rh + NZ - 1 - k, rh + 1 + k)
        row = jnp.where(n == 0, rh, lax.rem(row, NZ))
        return row, from_u

    xm1 = lax.rem(x + NX - 1, NX)
    xp1 = lax.rem(x + 1, NX)
    xp2 = lax.rem(x + 2, NX)

    def stage1(n, first):
        row, from_u = order(n)

        @pl.when(driver)
        def _():
            for j in range(2):
                if first:
                    @pl.when(pu < 5)
                    def _():
                        zcopy(row, 0, zu, j).start()

                    @pl.when(pd < 5)
                    def _():
                        zcopy(row, 8, zd, j).start()
                else:
                    arrived(row, x, j)

                    @pl.when(jnp.logical_and(from_u, pu < 5))
                    def _():
                        zcopy(row, n, zu, j).start()

                    @pl.when(jnp.logical_and(jnp.logical_not(from_u), pd < 5))
                    def _():
                        zcopy(row, n, zd, j).start()
                xcopy(n, 0, row, x, xr, j).start()
                xcopy(n, 1, row, x, xl, j).start()
                dcopy(row, x, j).start()

    def stage2(n):
        row, _ = order(n)

        @pl.when(driver)
        def _():
            even = lax.rem(row, 2) == 0
            for j in range(2):
                arrived(row, xm1, j)

                @pl.when(even)
                def _():
                    xcopy(n, 2, row, xm1, xr, j).start()
                dcopy(row, xm1, j).start()
                arrived(row, xp1, j)

                @pl.when(jnp.logical_not(even))
                def _():
                    xcopy(n, 2, row, xp1, xl, j).start()
                dcopy(row, xp1, j).start()

    def stage3(n):
        row, _ = order(n)

        @pl.when(driver)
        def _():
            for j in range(2):
                arrived(row, xp2, j)
                dcopy(row, xp2, j).start()

        @pl.when(foreign)
        def _():
            for col in range(NX):
                for j in range(2):
                    arrived(row, col, j)

    def hop(src, dst, slot, recv, dev):
        return [remote(src.at[j], dst.at[j], zs_sem.at[slot, j], recv.at[j], (dev, t))
                for j in range(2)]

    def land(row):
        return kv.at[row, x], kv_sem.at[row, x]

    own_down = hop(tr.at[0], land(r)[0], 0, land(r)[1], zd)
    own_up = hop(tr.at[0], land(r)[0], 0, land(r)[1], zu)
    hop_down = hop(tr.at[0], tr.at[1], 0, tr_sem, zd)
    hop_up = hop(tr.at[0], tr.at[1], 0, tr_sem, zu)
    fwd_down = hop(tr.at[1], land(5)[0], 1, land(5)[1], zd)
    fwd_up = hop(tr.at[1], land(6)[0], 1, land(6)[1], zu)

    q_sib = remote(qv.at[1], qin.at[0], qs_sem.at[0], q_sem.at[0], (s, sib))
    q_par = remote(qv.at[0], qin.at[1], qs_sem.at[0], q_sem.at[1], (part, t))
    q_pas = remote(qv.at[1], qin.at[1], qs_sem.at[1], q_sem.at[1], (part, sib))

    @pl.when(driver)
    def _():
        own_k.wait()
        own_v.wait()
        stage1(0, True)

    @pl.when(foreign)
    def _():
        tr_k.wait()
        tr_v.wait()
        for rr, cps in ((4, own_down), (5, hop_down), (6, hop_up), (7, own_up)):
            @pl.when(r == rr)
            def _():
                for cp in cps:
                    cp.start()

    q_lo.wait()
    q_hi.wait()

    @pl.when(driver)
    def _():
        q_sib.start()

    @pl.when(foreign)
    def _():
        for rr, cps in ((4, fwd_down), (7, fwd_up)):
            @pl.when(r == rr)
            def _():
                for j, cp in enumerate(cps):
                    b = tr.at[1, j]
                    pltpu.make_async_copy(b, b, tr_sem.at[j]).wait()
                    cp.start()
        q_par.start()
        q_pas.start()

    acc[...] = jnp.zeros_like(acc)
    mrow[...] = jnp.full_like(mrow, NEG)

    def split(src, a):
        for h in range(4):
            f = src[:, h * HEAD:(h + 1) * HEAD].astype(jnp.float32) * LOG2_SCALE
            hi = f.astype(jnp.bfloat16)
            lo = (f - hi.astype(jnp.float32)).astype(jnp.bfloat16)
            qhl[a, h] = jnp.concatenate([hi, lo], axis=1)

    @pl.when(driver)
    def _():
        split(qv.at[0], 0)

    @pl.when(foreign)
    def _():
        pltpu.make_async_copy(qin.at[0], qin.at[0], q_sem.at[0]).wait()
        split(qin.at[0], 0)

    def early(n, carry):
        stage1(n, False)

        @pl.when(n >= LEAD1 - LEAD2)
        def _():
            stage2(n - (LEAD1 - LEAD2))
        return carry

    lax.fori_loop(1, LEAD1, early, 0)

    def attend(a, row, pair, offset, masked):
        ks = kv[row, pl.ds(2 * pair, 2), 0].reshape(2 * ROWS, HEAD)
        vs = kv[row, pl.ds(2 * pair, 2), 1].reshape(2 * ROWS, HEAD)
        k2 = jnp.concatenate([ks, ks], axis=1)
        v1 = jnp.concatenate([vs, jnp.ones_like(vs)], axis=1)
        if masked:
            qpos = lax.broadcasted_iota(jnp.int32, (2 * ROWS, 2 * ROWS), 0)
            qpos = (qpos & (ROWS - 1)) + offset
            vis = qpos >= lax.broadcasted_iota(jnp.int32, (2 * ROWS, 2 * ROWS), 1)
        qs = [qhl[a, pl.ds(2 * h, 2)].reshape(2 * ROWS, 256) for h in range(2)]
        ms = [mrow[a, pl.ds(2 * h, 2)].reshape(2 * ROWS, 128) for h in range(2)]

        def scores(h):
            sc = lax.dot_general(qs[h], k2, (((1,), (1,)), ((), ())),
                                 preferred_element_type=jnp.float32)
            return jnp.where(vis, sc, NEG) if masked else sc

        done = []
        cur = scores(0)
        for h in range(2):
            nxt = scores(h + 1) if h < 1 else None
            mn = jnp.maximum(ms[h], jnp.max(cur, axis=1, keepdims=True))
            al = jnp.exp2(ms[h] - mn)
            p = jnp.exp2(cur - jnp.concatenate([mn] * 4, axis=1)).astype(jnp.bfloat16)
            pv = jnp.dot(p, v1, preferred_element_type=jnp.float32)
            done.append((mn, al, pv))
            cur = nxt
        for h in range(2):
            mn, al, pv = done[h]
            two = pl.ds(2 * h, 2)
            mrow[a, two] = mn.reshape(2, ROWS, 128)
            old = acc[a, two].reshape(2 * ROWS, 256)
            acc[a, two] = (old * jnp.concatenate([al, al], axis=1) + pv).reshape(2, ROWS, 256)

    def row_step(n, carry):
        @pl.when(n < NZ - LEAD1)
        def _():
            stage1(n + LEAD1, False)

        @pl.when(n < NZ - LEAD2)
        def _():
            stage2(n + LEAD2)

        @pl.when(n < NZ)
        def _():
            stage3(n)

        @pl.when(n == LATE)
        def _():
            pltpu.make_async_copy(qin.at[1], qin.at[1], q_sem.at[1]).wait()
            split(qin.at[1], 1)

        def sub(i, carry2):
            a = (i >= 2).astype(jnp.int32)
            pair = lax.rem(i, 2)
            last = jnp.minimum(n, 2 * (n - LATE) + 1)
            from_row = jnp.maximum(jnp.minimum(n - 1, 2 * (n - LATE) - 1) + 1, 0)
            m = jnp.where(i < 2, n, from_row + i // 2 - 1)
            live = m <= jnp.where(i < 2, n, last)
            row, _ = order(jnp.clip(m, 0, NZ - 1))
            zr = row + ch * (NZ - 1 - 2 * row)
            bq = s + a * (part - s)
            pos = 2 * zr + pair

            @pl.when(jnp.logical_and(live, pos < bq // 2))
            def _():
                attend(a, row, pair, 0, False)

            @pl.when(jnp.logical_and(live, pos == bq // 2))
            def _():
                attend(a, row, pair, lax.rem(bq, 2) * ROWS, True)
            return carry2

        lax.fori_loop(0, 6, sub, 0)
        return carry

    lax.fori_loop(0, NZ, row_step, 0)

    lane = lax.broadcasted_iota(jnp.int32, (8, 128), 1)
    base = (t - c + ch) * 8 + 4 * (1 - (c == ch).astype(jnp.int32))
    best = jnp.full((8, 128), -3e38, jnp.float32)
    for h in range(4):
        both = jnp.maximum(mrow[0, h], mrow[1, h])
        top = jnp.max(both, axis=0, keepdims=True) * math.log(2.0)
        best = jnp.where(lane == base + h, jnp.broadcast_to(top, (8, 128)), best)
    mx_out[0] = best

    for a in (1, 0):
        for h in range(4):
            res[a, :, pl.ds(h * HEAD, HEAD)] = (
                acc[a, h, :, :HEAD] / acc[a, h, :, HEAD:]).astype(jnp.bfloat16)

    lo_cols = o_hbm.at[:, pl.ds(0, 512)]
    hi_cols = o_hbm.at[:, pl.ds(512, 512)]
    back_d = remote(res.at[1], lo_cols, os_sem.at[1], o_sem.at[0], (part, t))
    back_s = remote(res.at[1], hi_cols, os_sem.at[1], o_sem.at[1], (part, sib))
    keep_d = pltpu.make_async_copy(res.at[0], lo_cols, os_sem.at[0])
    keep_s = remote(res.at[0], hi_cols, os_sem.at[0], o_sem.at[1], (s, sib))

    @pl.when(driver)
    def _():
        back_d.start()
        keep_d.start()

    @pl.when(foreign)
    def _():
        back_s.start()
        keep_s.start()

    at = 0
    for rnd, peers in enumerate((row_peers, ring_peers, y_peers)):
        sends = [remote(mx_out.at[rnd], mx_in.at[at + i], ms_sem.at[at + i], mr_sem.at[at + i], dev)
                 for i, dev in enumerate(peers)]
        for cp in sends:
            cp.start()
        best = mx_out[rnd]
        for i, cp in enumerate(sends):
            cp.wait_recv()
            best = jnp.maximum(best, mx_in[at + i])
        if rnd < 2:
            mx_out[rnd + 1] = best
        at += len(peers)
    for i in range(at):
        remote(mx_out.at[0], mx_in.at[i], ms_sem.at[i], mr_sem.at[i], (s, sib)).wait_send()
    hm_ref[...] = jnp.broadcast_to(best[0:1], (128, 128)).T

    @pl.when(driver)
    def _():
        for j in range(2):
            @pl.when(pu < 5)
            def _():
                zcopy(r, 0, zu, j).wait_send()

            @pl.when(pd < 5)
            def _():
                zcopy(r, 8, zd, j).wait_send()

        def drain(n, carry):
            row, from_u = order(n)
            for j in range(2):
                @pl.when(jnp.logical_and(n > 0, jnp.logical_and(from_u, pu < 5)))
                def _():
                    zcopy(row, n, zu, j).wait_send()

                @pl.when(jnp.logical_and(n > 0, jnp.logical_and(jnp.logical_not(from_u), pd < 5)))
                def _():
                    zcopy(row, n, zd, j).wait_send()
                xcopy(n, 0, row, x, xr, j).wait_send()
                xcopy(n, 1, row, x, xl, j).wait_send()
                xcopy(n, 2, row, xm1, xr, j).wait_send()
                for col in range(NX):
                    dcopy(row, col, j).wait_send()
            return carry

        lax.fori_loop(0, NZ, drain, 0)
        q_sib.wait_send()
        back_d.wait_send()
        keep_d.wait()
        keep_s.wait_recv()

    @pl.when(foreign)
    def _():
        for cp in own_down:
            cp.wait_send()

        @pl.when(jnp.logical_or(r == 4, r == 7))
        def _():
            for cp in fwd_down:
                cp.wait_send()
        q_par.wait_send()
        q_pas.wait_send()
        back_s.wait_send()
        keep_s.wait_send()
        back_d.wait_recv()
        back_s.wait_recv()


def attend_all(q, k, v):
    bf = jnp.bfloat16
    return pl.pallas_call(
        attention_kernel,
        out_shape=(jax.ShapeDtypeStruct((ROWS, 1024), bf),
                   jax.ShapeDtypeStruct((128, 128), jnp.float32)),
        in_specs=[pl.BlockSpec(memory_space=pl.ANY)] * 3,
        out_specs=(pl.BlockSpec(memory_space=pl.ANY),
                   pl.BlockSpec(memory_space=pltpu.VMEM)),
        scratch_shapes=[
            pltpu.VMEM((2, ROWS, 512), bf),
            pltpu.VMEM((NZ, NX, 2, ROWS, HEAD), bf),
            pltpu.VMEM((2, 2, ROWS, HEAD), bf),
            pltpu.VMEM((2, ROWS, 512), bf),
            pltpu.VMEM((2, 4, ROWS, 256), bf),
            pltpu.VMEM((2, 4, ROWS, 256), jnp.float32),
            pltpu.VMEM((2, 4, ROWS, 128), jnp.float32),
            pltpu.VMEM((2, ROWS, 512), bf),
            pltpu.SemaphoreType.DMA((4,)),
            pltpu.SemaphoreType.DMA((NZ, NX, 2)),
            pltpu.SemaphoreType.DMA((2,)),
            pltpu.SemaphoreType.DMA((2,)),
            pltpu.SemaphoreType.DMA((2,)),
            pltpu.SemaphoreType.DMA((9, 2)),
            pltpu.SemaphoreType.DMA((NZ, 3, 2)),
            pltpu.SemaphoreType.DMA((NZ, NX, 2)),
            pltpu.SemaphoreType.DMA((2,)),
            pltpu.SemaphoreType.DMA((2,)),
            pltpu.VMEM((3, 8, 128), jnp.float32),
            pltpu.VMEM((17, 8, 128), jnp.float32),
            pltpu.SemaphoreType.DMA((17,)),
            pltpu.SemaphoreType.DMA((17,)),
        ],
        compiler_params=pltpu.CompilerParams(
            collective_id=0, has_side_effects=True, vmem_limit_bytes=67043328),
        name="attend",
    )(q, k, v)


def scale_kernel(hm_ref, w_hbm, kw_hbm, att_hbm, wo_hbm, ko_hbm, ao_hbm, top_ref,
                 w_v, kw_v, att_v, in_sem, out_sem):
    t = lax.axis_index("tp")
    loads = [pltpu.make_async_copy(src, dst, in_sem.at[i]) for i, (src, dst) in enumerate(
        ((kw_hbm, kw_v), (w_hbm, w_v), (att_hbm, att_v)))]
    stores = [pltpu.make_async_copy(src, dst, out_sem.at[i]) for i, (src, dst) in enumerate(
        ((kw_v, ko_hbm), (w_v, wo_hbm), (att_v, ao_hbm)))]
    for cp in loads:
        cp.start()
    mine = hm_ref[pl.ds(pl.multiple_of(8 * t, 8), 8), :]
    root = jnp.sqrt(TAU / jnp.maximum(jnp.max(mine, axis=0, keepdims=True), TAU))
    gamma = (TAU / jnp.maximum(mine, TAU)) / root
    clips = []
    for g in range(8):
        most = jnp.max(hm_ref[pl.ds(8 * g, 8), :], axis=0, keepdims=True)
        clips.append(jnp.sqrt(TAU / jnp.maximum(most, TAU)))
    loads[0].wait()
    for g in range(8):
        cols = slice(g * HEAD, (g + 1) * HEAD)
        kw_v[:, cols] = (kw_v[:, cols].astype(jnp.float32) * clips[g]).astype(jnp.bfloat16)
    stores[0].start()
    loads[1].wait()
    for h in range(8):
        cols = slice(h * HEAD, (h + 1) * HEAD)
        w_v[:, cols] = (w_v[:, cols].astype(jnp.float32) * gamma[h:h + 1]).astype(jnp.bfloat16)
    stores[1].start()
    loads[2].wait()
    stores[2].start()
    lane = lax.broadcasted_iota(jnp.int32, (1, 128), 1)
    row = jnp.zeros((1, 128), jnp.float32)
    for h in range(8):
        row = jnp.where(lane == h, mine[h:h + 1, :], row)
    top_ref[...] = row[:, :8]
    for cp in stores:
        cp.wait()


def scale(hm, w, kw, att):
    vm = pl.BlockSpec(memory_space=pltpu.VMEM)
    hbm = pl.BlockSpec(memory_space=pl.ANY)
    full = jax.ShapeDtypeStruct(w.shape, w.dtype)
    return pl.pallas_call(
        scale_kernel,
        out_shape=(full, full, full, jax.ShapeDtypeStruct((1, 8), jnp.float32)),
        in_specs=[vm, hbm, hbm, hbm], out_specs=(hbm, hbm, hbm, vm),
        scratch_shapes=[pltpu.VMEM(w.shape, w.dtype)] * 3 + [pltpu.SemaphoreType.DMA((3,))] * 2,
        compiler_params=pltpu.CompilerParams(vmem_limit_bytes=67043328),
        name="scale",
    )(hm, w, kw, att)


def shards(q, k, v, w, kw):
    out, hm = attend_all(q, k, v)
    w_out, k_out, att, top = scale(hm, w, kw, out)
    return att, top.reshape(8), w_out, k_out


def solution(mesh):
    in_specs = (P("seq", "tp"), P("seq", "tp"), P("seq", "tp"), P("seq", "tp"), P("seq", None))
    out_specs = (P("seq", "tp"), P("tp"), P("seq", "tp"), P("seq", None))
    return jax.shard_map(shards, mesh=mesh, in_specs=in_specs, out_specs=out_specs, check_vma=False)
```
